32 devices in a mesh: gx: 4 (over y, core), gy: 8 (over z, x).
Axes of the slice: x: 2, y: 2, z: 4, core: 2. Of those that a mesh axis runs over, the one named last changes fastest.
Arguments:
- tokens: bfloat16 [4, 256, 6144], P('gx', None, 'gy'), may hold values from -6 to 6
- norm_gain: float32 [6144], replicated, may hold values from 0.1 to 1.9
- qkv_weight: bfloat16 [6144, 3, 4096], P('gx', None, 'gy'), may hold values from -0.078125 to 0.078125
- up_weight: bfloat16 [6144, 24576], P('gx', 'gy'), may hold values from -0.078125 to 0.078125
- query_gain: float32 [128], replicated, may hold values from 0.1 to 1.9
- key_gain: float32 [128], replicated, may hold values from 0.1 to 1.9
- out_weight: bfloat16 [4096, 6144], P('gy', 'gx'), may hold values from -0.09375 to 0.09375
- down_weight: bfloat16 [24576, 6144], P('gy', 'gx'), may hold values from -0.0390625 to 0.0390625
- attention_keep: int32 [4, 256, 6144], P('gx', None, 'gy'), may hold values 0 or 1
- feedforward_keep: int32 [4, 256, 6144], P('gx', None, 'gy'), may hold values 0 or 1
Outputs:
- block_out: bfloat16 [4, 256, 6144], P('gx', None, 'gy')
The draws below stay inside these ranges and needn't reach their ends.
All inputs are finite; a program needn't handle non-finite values. No bound on the sum of `attention_keep` or of `feedforward_keep` on one device may be relied on, other than what follows from the above.
Results may differ from the reference program's by a relative error of at most 0.017.
Values may be sent and summed in bfloat16 or wider, within the bound.
A program may use at most 128 MiB of HBM per device.

```python
import jax
import jax.numpy as jnp
from jax import lax

D = 6144
HEADS = 32
HDIM = 128
FF = 24576
SEQ = 256
IMAGES = 4
INNER = 4096
N_GX = 4
N_GY = 8


def place_ends(entries, key, low, top_value):
    longest = entries.shape.index(max(entries.shape))
    spots = []
    for shift in (0, 1):
        where = [jax.random.randint(jax.random.fold_in(key, axis), (), 0, length) for axis, length in enumerate(entries.shape)]
        where[longest] = (where[longest] + shift) % entries.shape[longest]
        spots.append(tuple(where))
    return entries.at[spots[0]].set(low).at[spots[1]].set(top_value)


def steps_of(stream_key, dims, split, low, largest):
    level, own = 1.0, jax.random.fold_in(stream_key, 6)
    for dim, shards_of in split:
        steps = jnp.exp(jax.random.uniform(jax.random.fold_in(own, dim), (shards_of,), jnp.float32, low / len(split), largest / len(split)))
        level = level * jnp.repeat(steps, dims[dim] // shards_of).reshape([-1 if axis == dim else 1 for axis in range(len(dims))])
    return level


def scatter_about(rng, extent, spread, limit, cuts=(), kind=jnp.bfloat16):
    values = spread * jax.random.normal(rng, extent, jnp.float32)
    if cuts:
        values = values * steps_of(rng, extent, cuts, -0.22, 0.18)
    return jnp.clip(values, -limit, limit).astype(kind)


def setup_inputs(seed: int = 0) -> dict:
    key_of = jax.random.split(jax.random.key(seed), 11)
    return {
        "tokens": scatter_about(key_of[0], (IMAGES, SEQ, D), 1.0, 6.0, ((0, 4), (2, 8))),
        "norm_gain": jnp.clip(1.0 + 0.18 * jax.random.normal(key_of[1], (D,), jnp.float32), 0.1, 1.9),
        "qkv_weight": scatter_about(key_of[2], (D, 3, INNER), D ** -0.5, 0.078125, ((0, 4), (2, 8))),
        "up_weight": scatter_about(key_of[3], (D, FF), D ** -0.5, 0.078125, ((0, 4), (1, 8))),
        "query_gain": jnp.clip(1.0 + 0.18 * jax.random.normal(key_of[4], (HDIM,), jnp.float32), 0.1, 1.9),
        "key_gain": jnp.clip(1.0 + 0.18 * jax.random.normal(key_of[5], (HDIM,), jnp.float32), 0.1, 1.9),
        "out_weight": scatter_about(key_of[6], (INNER, D), INNER ** -0.5, 0.09375, ((0, 8), (1, 4))),
        "down_weight": scatter_about(key_of[7], (FF, D), FF ** -0.5, 0.0390625, ((0, 8), (1, 4))),
        "attention_keep": place_ends((jax.random.randint(key_of[8], (IMAGES, SEQ, D), 0, 10) < 9).astype(jnp.int32), jax.random.fold_in(key_of[8], 1), 0, 1),
        "feedforward_keep": place_ends((jax.random.randint(key_of[9], (IMAGES, SEQ, D), 0, 10) < 9).astype(jnp.int32), jax.random.fold_in(key_of[9], 1), 0, 1),
    }


epsilon = 1e-06
keep_scale = 1.0 / 0.9

def layer_norm(values, gain):
    center = values - lax.optimization_barrier(jnp.mean(values, axis=-1, keepdims=True))
    variance = lax.optimization_barrier(jnp.mean(center * center, axis=-1, keepdims=True))
    return center * lax.rsqrt(variance + epsilon) * gain

def head_norm(values, gain):
    row_count = values.shape[0]
    shaped = values.reshape(row_count, -1, gain.shape[0])
    return layer_norm(shaped, gain).reshape(row_count, -1)

def rounded_sum(left, right, block_width, count):

    def accumulate(running, index):
        offset = index * block_width
        segment = lax.dynamic_slice_in_dim(left, offset, block_width, 1)
        rows_part = lax.dynamic_slice_in_dim(right, offset, block_width, 0)
        term = jnp.dot(segment, rows_part, preferred_element_type=jnp.float32).astype(jnp.bfloat16)
        term = lax.optimization_barrier(term)
        return (running + term.astype(jnp.float32), None)
    begin = jnp.zeros((left.shape[0], right.shape[1]), jnp.float32)
    total, unused = lax.scan(accumulate, begin, jnp.arange(count, dtype=jnp.int32))
    return total

def reference(tokens, norm_gain, qkv_weight, up_weight, query_gain, key_gain, out_weight, down_weight, attention_keep, feedforward_keep):
    row_total = IMAGES * SEQ
    inner = HEADS * HDIM
    normed = layer_norm(tokens.astype(jnp.float32), norm_gain).astype(jnp.bfloat16).reshape(row_total, D)
    joined = jnp.concatenate([qkv_weight.reshape(D, 3 * inner), up_weight], axis=1)
    united = rounded_sum(normed, joined, D // N_GX, N_GX)
    queries = head_norm(united[:, :inner], query_gain).astype(jnp.bfloat16)
    keys = head_norm(united[:, inner:2 * inner], key_gain).astype(jnp.bfloat16)
    values = united[:, 2 * inner:3 * inner].astype(jnp.bfloat16)
    query_grid = queries.reshape(IMAGES, SEQ, HEADS, HDIM).astype(jnp.float32)
    key_grid = keys.reshape(IMAGES, SEQ, HEADS, HDIM).astype(jnp.float32)
    value_grid = values.reshape(IMAGES, SEQ, HEADS, HDIM).astype(jnp.float32)
    scores = jnp.einsum('bshd,bthd->bhst', query_grid, key_grid) * HDIM ** (-0.5)
    raised = jnp.exp(scores)
    weights = (raised / lax.optimization_barrier(jnp.sum(raised, axis=-1, keepdims=True))).astype(jnp.bfloat16)
    attended = jnp.einsum('bhst,bthd->bshd', weights.astype(jnp.float32), value_grid)
    attended = attended.astype(jnp.bfloat16).reshape(row_total, inner)
    hidden = jax.nn.gelu(united[:, 3 * inner:], approximate=False).astype(jnp.bfloat16)
    attention_out = rounded_sum(attended, out_weight, inner // N_GY, N_GY).reshape(IMAGES, SEQ, D)
    feedforward_out = rounded_sum(hidden, down_weight, FF // N_GY, N_GY).reshape(IMAGES, SEQ, D)
    branches = attention_keep.astype(jnp.float32) * attention_out + feedforward_keep.astype(jnp.float32) * feedforward_out
    return (tokens.astype(jnp.float32) + branches * keep_scale).astype(jnp.bfloat16)
```

```python
import functools

import jax
import jax.numpy as jnp
from jax import lax
from jax.experimental import pallas as pl
from jax.experimental.pallas import tpu as pltpu
from jax.sharding import PartitionSpec as P

epsilon = 1e-06
keep_scale = 1.0 / 0.9
UP_CHUNKS = 2

f32 = jnp.float32
bf16 = jnp.bfloat16


def layer_norm(values, gain):
    center = values - jnp.mean(values, axis=-1, keepdims=True)
    variance = jnp.mean(center * center, axis=-1, keepdims=True)
    return center * lax.rsqrt(variance + epsilon) * gain


def head_norm(values, gain):
    row_count = values.shape[0]
    shaped = values.reshape(row_count, -1, gain.shape[0])
    return layer_norm(shaped, gain).reshape(row_count, -1)


def mul(left, right):
    return jnp.dot(left, right, preferred_element_type=f32)


def swap(values, bit, n_gx):
    return lax.ppermute(values, "gx", [(i, i ^ bit) for i in range(n_gx)])


def scatter_sum(odd_rows, even_rows, weight, n_gx):
    received = swap(mul(odd_rows, weight).astype(bf16), 1, n_gx)
    total = mul(even_rows, weight).astype(bf16).astype(f32) + received.astype(f32)
    bit, width = 2, weight.shape[1]
    own_rows = 2 * odd_rows.shape[0] // n_gx
    while bit < n_gx:
        pairs = total.reshape(-1, 2, own_rows, width)
        received = swap(pairs[:, 1].astype(bf16), bit, n_gx)
        total = pairs[:, 0] + received.astype(f32)
        bit *= 2
    return total.reshape(own_rows, width)


def gather_pair(own, n_gx):
    held, bit = own, n_gx // 2
    while bit > 1:
        held = jnp.concatenate([held, swap(held, bit, n_gx)], axis=0)
        bit //= 2
    return held, swap(held, 1, n_gx)


def gather_order(n_gx):
    order, bit = [0], n_gx // 2
    while bit >= 1:
        order = order + [p ^ bit for p in order]
        bit //= 2
    return order


def ring_place(index, count):
    return jnp.where(index % 2 == 0, index // 2, count - 1 - index // 2)


def ring_gather(own, ring, place):
    n = len(ring)
    ahead = [(ring[r], ring[(r + 1) % n]) for r in range(n)]
    back = [(b, a) for a, b in ahead]
    forward, backward = [own], [own]
    for step in range(n // 2 - 1):
        forward.append(lax.ppermute(forward[-1], "gy", ahead))
        backward.append(lax.ppermute(backward[-1], "gy", back))
    half = own.shape[0] // 2
    far = jnp.concatenate(
        [
            lax.ppermute(forward[-1][:half], "gy", ahead),
            lax.ppermute(backward[-1][half:], "gy", back),
        ],
        axis=0,
    )
    return jnp.stack(forward + [far] + backward[:0:-1])


def ring_scatter(partial, ring, place):
    n = len(ring)
    half = partial.shape[1] // 2
    ahead = [(ring[r], ring[(r + 1) % n]) for r in range(n)]
    back = [(b, a) for a, b in ahead]

    def block(index, start):
        index = lax.rem(index + 2 * n, n)
        return lax.dynamic_slice(
            partial, (index, start, 0), (1, half, partial.shape[2])
        )[0]

    up, down = block(place - 1, 0), block(place + 1, half)
    for step in range(n - 1):
        came_up = lax.ppermute(up, "gy", ahead)
        came_down = lax.ppermute(down, "gy", back)
        up = came_up.astype(f32) + block(place - 2 - step, 0).astype(f32)
        down = came_down.astype(f32) + block(place + 2 + step, half).astype(f32)
        up, down = up.astype(bf16), down.astype(bf16)
    return jnp.concatenate([up, down], axis=0)


def per_device(
    tokens,
    norm_gain,
    qkv_weight,
    up_weight,
    query_gain,
    key_gain,
    out_weight,
    down_weight,
    attention_keep,
    feedforward_keep,
):
    n_gx, n_gy = lax.axis_size("gx"), lax.axis_size("gy")
    sub = n_gy // n_gx
    me = lax.axis_index("gx")
    ring = list(range(0, n_gy, 2)) + list(range(1, n_gy, 2))[::-1]
    place = ring_place(lax.axis_index("gy"), n_gy)
    images, seq_len, slice_width = tokens.shape
    own_rows = images * seq_len
    block_width = qkv_weight.shape[0]
    head_cols = qkv_weight.shape[2]
    head_size = query_gain.shape[0]

    flat = tokens.reshape(own_rows, slice_width)
    turned = lax.ppermute(
        flat,
        ("gx", "gy"),
        [
            (i * n_gy + k * sub + s, k * n_gy + i * sub + s)
            for i in range(n_gx)
            for k in range(n_gx)
            for s in range(sub)
        ],
    )
    gathered = ring_gather(turned, ring, place)

    wide = flat.astype(f32)
    mean = jnp.mean(wide, axis=1)
    squares = jnp.sum((wide - mean[:, None]) ** 2, axis=1)
    count, bit = slice_width, 1
    while bit < n_gy:
        pairs = [(i, i ^ bit) for i in range(n_gy)]
        other = lax.ppermute(jnp.stack([mean, squares]), "gy", pairs)
        squares = squares + other[1] + (0.5 * count) * (mean - other[0]) ** 2
        mean = 0.5 * (mean + other[0])
        count, bit = 2 * count, 2 * bit
    stats = jnp.stack([mean, lax.rsqrt(squares / count + epsilon)])[None]
    bit = 1
    while bit < n_gx:
        stats = jnp.concatenate([stats, swap(stats, bit, n_gx)], axis=0)
        bit *= 2
    gain = lax.dynamic_slice_in_dim(norm_gain, me * block_width, block_width, 0)

    def normed_rows(position):
        image = me ^ position
        rows = jnp.concatenate(
            [
                lax.dynamic_index_in_dim(
                    gathered,
                    lax.rem(place - ring_place(image * sub + s, n_gy) + n_gy, n_gy),
                    0,
                    keepdims=False,
                )
                for s in range(sub)
            ],
            axis=1,
        ).astype(f32)
        row_mean, row_scale = stats[position, 0], stats[position, 1]
        return ((rows - row_mean[:, None]) * row_scale[:, None] * gain).astype(bf16)

    odd_rows = jnp.concatenate([normed_rows(p) for p in range(1, n_gx, 2)], axis=0)
    even_rows = jnp.concatenate([normed_rows(p) for p in range(0, n_gx, 2)], axis=0)

    qkv_flat = qkv_weight.reshape(block_width, 3 * head_cols)
    united = scatter_sum(odd_rows, even_rows, qkv_flat, n_gx)
    up_cols = up_weight.shape[1] // UP_CHUNKS
    hidden = []
    for c in range(UP_CHUNKS):
        total = scatter_sum(
            odd_rows, even_rows, up_weight[:, c * up_cols : (c + 1) * up_cols], n_gx
        )
        hidden.append(jax.nn.gelu(total, approximate=False).astype(bf16))

    queries = head_norm(united[:, :head_cols], query_gain).astype(bf16)
    keys = head_norm(united[:, head_cols : 2 * head_cols], key_gain).astype(bf16)
    values = united[:, 2 * head_cols :].astype(bf16)
    query_grid = queries.reshape(images, seq_len, -1, head_size)
    key_grid = keys.reshape(images, seq_len, -1, head_size)
    value_grid = values.reshape(images, seq_len, -1, head_size)
    scores = jnp.einsum(
        "bshd,bthd->bhst", query_grid, key_grid, preferred_element_type=f32
    ) * head_size ** (-0.5)
    raised = jnp.exp(scores)
    weights = (raised / jnp.sum(raised, axis=-1, keepdims=True)).astype(bf16)
    attended = jnp.einsum("bhst,bthd->bshd", weights, value_grid, preferred_element_type=f32)
    attended = attended.astype(bf16).reshape(own_rows, head_cols)

    order = gather_order(n_gx)
    def home(devices):
        return [
            (
                k * n_gy + devices[s * n_gx + q],
                (k ^ order[q]) * n_gy + k * sub + s,
            )
            for k in range(n_gx)
            for s in range(sub)
            for q in range(n_gx)
        ]

    def columns(weight, s):
        return weight[:, s * slice_width : (s + 1) * slice_width]

    attended_halves = gather_pair(attended, n_gx)
    attention_out = lax.psum_scatter(
        jnp.concatenate(
            [
                mul(rows, columns(out_weight, s)).astype(bf16)
                for s in range(sub)
                for rows in attended_halves
            ],
            axis=0,
        ),
        "gy",
        scatter_dimension=0,
        tiled=True,
    )
    attention_out = lax.ppermute(attention_out, ("gx", "gy"), home(range(n_gy))).astype(f32)
    hidden_halves = [gather_pair(part, n_gx) for part in hidden]
    pieces = []
    for s in range(sub):
        for half in range(2):
            total = 0.0
            for c in range(UP_CHUNKS):
                weight = down_weight[c * up_cols : (c + 1) * up_cols]
                total = total + mul(hidden_halves[c][half], columns(weight, s))
            pieces.append(total.astype(bf16))
    partial = jnp.concatenate(pieces, axis=0).reshape(n_gy, own_rows, slice_width)
    feedforward_out = ring_scatter(partial, ring, place)
    feedforward_out = lax.ppermute(feedforward_out, ("gx", "gy"), home(ring)).astype(f32)

    shape = tokens.shape
    branches = attention_keep.astype(f32) * attention_out.reshape(
        shape
    ) + feedforward_keep.astype(f32) * feedforward_out.reshape(shape)
    return (tokens.astype(f32) + branches * keep_scale).astype(bf16)


MESH = pl.DeviceIdType.MESH
VMEM_LIMIT = 67043328
GATHER_PIECES = 2
ROW_STEP = 64


def flip(index, mask):
    for bit in (1, 2):
        if mask & bit:
            index = index + bit - 2 * bit * ((index // bit) % 2)
    return index


def remote(src, dst, send_sem, recv_sem, device):
    return pltpu.make_async_remote_copy(
        src_ref=src,
        dst_ref=dst,
        send_sem=send_sem,
        recv_sem=recv_sem,
        device_id=device,
        device_id_type=MESH,
    )


def over_rows(count, body):
    def step(i, carry):
        body(pl.ds(pl.multiple_of(i * ROW_STEP, ROW_STEP), ROW_STEP))
        return carry

    lax.fori_loop(0, count // ROW_STEP, step, 0)


def aligned(start, size):
    return pl.ds(pl.multiple_of(start, size), size)


def block_kernel(
    n_gy,
    tokens,
    gain,
    query_gain,
    key_gain,
    qkv_hbm,
    up_hbm,
    out_hbm,
    down_hbm,
    attention_keep,
    feedforward_keep,
    result,
    *scratch,
):
    (
        w_in,
        w_down,
        w_out,
        keeps,
        stat_own,
        stat_all,
        normed,
        rows_in,
        part,
        part_in,
        kept,
        cross,
        cross_in,
        hid,
        att,
        branch,
        branch_in,
        line_out,
        line_low,
        line_high,
        running,
        final,
        in_sem,
        down_sem,
        out_sem,
        keep_sem,
        stat_send,
        stat_recv,
        first_send,
        gather_recv,
        gather_send,
        side_send,
        side_recv,
        part_send,
        part_recv,
        cross_send,
        cross_recv,
        share_send,
        share_recv,
        branch_send,
        branch_recv,
        line_send,
        low_recv,
        high_recv,
        final_recv,
        branch_credit,
        line_credit,
    ) = scratch
    n_gx = 4
    sub = n_gy // n_gx
    g, j = lax.axis_index("gx"), lax.axis_index("gy")
    z, x = j // sub, j % sub
    core, across, side = (flip(g, 1), j), (flip(g, 2), j), (g, j + 1 - 2 * x)
    seq, slice_width = normed.shape
    features = n_gy * slice_width
    head = query_gain.shape[1]
    quarter_head, quarter_ff = att.shape[2] // n_gx, hid.shape[2] // n_gx
    quarter = part.shape[2]
    chunks = n_gx
    step_rows = seq // GATHER_PIECES
    own_cols, side_cols = pl.ds(0, slice_width), pl.ds(slice_width, slice_width)

    relative = (3, 2, 1, 0)
    in_copies, down_copies, out_copies = [], [], []
    for q, r in enumerate(relative):
        k = flip(g, r)
        copies = []
        for h in range(2):
            from_rows = aligned(slice_width * (x if h == 0 else 1 - x), slice_width)
            to_rows = pl.ds(h * slice_width, slice_width)
            for t in range(3):
                copies.append(
                    (
                        qkv_hbm.at[t, from_rows, aligned(k * quarter_head, quarter_head)],
                        w_in.at[q, to_rows, pl.ds(t * quarter_head, quarter_head)],
                    )
                )
            copies.append(
                (
                    up_hbm.at[from_rows, aligned(k * quarter_ff, quarter_ff)],
                    w_in.at[q, to_rows, pl.ds(3 * quarter_head, quarter_ff)],
                )
            )
        in_copies.append(
            [
                pltpu.make_async_copy(a, b, in_sem.at[q, n])
                for n, (a, b) in enumerate(copies)
            ]
        )
    for s in range(2):
        from_cols = aligned(slice_width * (1 - x if s == 0 else x), slice_width)
        for r in range(n_gx):
            k = flip(g, r)
            down_copies.append(
                pltpu.make_async_copy(
                    down_hbm.at[aligned(k * quarter_ff, quarter_ff), from_cols],
                    w_down.at[s, pl.ds(r * quarter_ff, quarter_ff)],
                    down_sem.at[s, r],
                )
            )
            out_copies.append(
                pltpu.make_async_copy(
                    out_hbm.at[aligned(k * quarter_head, quarter_head), from_cols],
                    w_out.at[s, pl.ds(r * quarter_head, quarter_head)],
                    out_sem.at[s, r],
                )
            )
    keep_copies = [
        pltpu.make_async_copy(attention_keep, keeps.at[0], keep_sem.at[0]),
        pltpu.make_async_copy(feedforward_keep, keeps.at[1], keep_sem.at[1]),
    ]
    for copies in in_copies:
        for copy in copies:
            copy.start()
    for copy in down_copies + out_copies + keep_copies:
        copy.start()

    barrier = pltpu.get_barrier_semaphore()
    for r in range(1, n_gx):
        pl.semaphore_signal(
            barrier, inc=1, device_id=(flip(g, r), j), device_id_type=MESH
        )
    for d in range(1, n_gy):
        pl.semaphore_signal(
            barrier, inc=1, device_id=(g, (j + d) % n_gy), device_id_type=MESH
        )

    wide = tokens[0].astype(f32)
    mean = jnp.mean(wide, axis=1, keepdims=True)
    squares = jnp.sum((wide - mean) ** 2, axis=1, keepdims=True)
    mean_row = jnp.transpose(jnp.broadcast_to(mean, (seq, 128)))[:8]
    squares_row = jnp.transpose(jnp.broadcast_to(squares, (seq, 128)))[:8]
    top = lax.broadcasted_iota(jnp.int32, (8, seq), 0) == 0
    stats = jnp.where(top, mean_row, squares_row)
    stat_own[...] = stats
    stat_all[0] = stats
    pl.semaphore_wait(barrier, n_gx + n_gy - 2)
    stat_copies = [
        remote(
            stat_own,
            stat_all.at[d],
            stat_send.at[d],
            stat_recv.at[d],
            (g, (j + d) % n_gy),
        )
        for d in range(1, n_gy)
    ]
    for copy in stat_copies:
        copy.start()
    for copy in stat_copies:
        copy.wait_recv()
    means = [stat_all[d, 0:1] for d in range(n_gy)]
    total_mean = sum(means) * (1.0 / n_gy)
    spread = sum((m - total_mean) ** 2 for m in means) * float(slice_width)
    spread = spread + sum(stat_all[d, 1:2] for d in range(n_gy))
    scale = lax.rsqrt(spread * (1.0 / features) + epsilon)
    mean_col = jnp.transpose(jnp.broadcast_to(total_mean, (128, seq)))
    scale_col = jnp.transpose(jnp.broadcast_to(scale, (128, seq)))
    for c0 in range(0, slice_width, 128):
        cols = slice(c0, c0 + 128)
        centre = tokens[0, :, cols].astype(f32) - mean_col
        normed[:, cols] = (centre * scale_col * gain[j, :, cols]).astype(bf16)

    at_root = g == z
    first_copies = [
        remote(
            normed.at[pl.ds(p * step_rows, step_rows)],
            rows_in.at[g, pl.ds(p * step_rows, step_rows), own_cols],
            first_send.at[p],
            gather_recv.at[g, p],
            (z, j),
        )
        for p in range(GATHER_PIECES)
    ]

    @pl.when(at_root)
    def _():
        rows_in[g, :, own_cols] = normed[...]

    @pl.when(jnp.logical_not(at_root))
    def _():
        for copy in first_copies:
            copy.start()

    goes_down = jnp.logical_and(z <= g, z > 0)
    goes_up = jnp.logical_and(z >= g, z < n_gx - 1)

    def gather_ref(c, p, cols):
        return rows_in.at[c, pl.ds(p * step_rows, step_rows), cols]

    def gather_copies(c, p):
        own = gather_ref(c, p, own_cols)
        down = remote(
            own, own, gather_send.at[0, c, p], gather_recv.at[c, p], (g, j - sub)
        )
        up = remote(
            own, own, gather_send.at[1, c, p], gather_recv.at[c, p], (g, j + sub)
        )
        beside = remote(
            own,
            gather_ref(c, p, side_cols),
            side_send.at[c, p],
            side_recv.at[c, p],
            side,
        )
        return down, up, beside

    def gather(c):
        for p in range(GATHER_PIECES):
            down, up, beside = gather_copies(c, p)

            @pl.when(jnp.logical_not(jnp.logical_and(at_root, g == c)))
            def _():
                up.wait_recv()

            @pl.when(goes_up)
            def _():
                up.start()

            @pl.when(goes_down)
            def _():
                down.start()

            beside.start()

    def gathered(c):
        for p in range(GATHER_PIECES):
            gather_copies(c, p)[2].wait_recv()

    def part_copy(c, half):
        return remote(
            part.at[2 * half],
            part_in.at[c % 2, half],
            part_send.at[c, half],
            part_recv.at[c, half],
            core,
        )

    def cross_copy(c):
        return remote(
            cross.at[c % 2], cross_in.at[c], cross_send.at[c], cross_recv.at[c], across
        )

    def project(c, half):
        if c == 0:
            for copy in in_copies[2 * half] + in_copies[2 * half + 1]:
                copy.wait()
        else:
            part_copy(c - 1, half).wait_send()

        def one(i, carry):
            q = 2 * half + i
            for n0 in range(0, quarter, 256):
                n1 = min(n0 + 256, quarter)
                part[q, :, n0:n1] = mul(rows_in[c], w_in[q, :, n0:n1]).astype(bf16)

            @pl.when(i == 0)
            def _():
                part_copy(c, half).start()

            return carry

        lax.fori_loop(0, 2, one, 0)

    def exchange(c):
        gathered(c)
        project(c, 0)
        part_copy(c, 0).wait_recv()
        if c >= 2:
            cross_copy(c - 2).wait_send()

        def to_cross(rows):
            total = part[1, rows].astype(f32) + part_in[c % 2, 0, rows].astype(f32)
            cross[c % 2, rows] = total.astype(bf16)

        over_rows(seq, to_cross)
        cross_copy(c).start()
        project(c, 1)
        part_copy(c, 1).wait_recv()

        def to_kept(rows):
            kept[c % 2, rows] = part[3, rows].astype(f32) + part_in[
                c % 2, 1, rows
            ].astype(f32)

        over_rows(seq, to_kept)

    def share_copies(c, which):
        held, width = (hid, quarter_ff) if which == 0 else (att, quarter_head)

        def slot(r):
            return held.at[c, :, pl.ds(r * width, width)]

        return [
            remote(
                slot(a),
                slot(b),
                share_send.at[c, which, n],
                share_recv.at[c, which, n],
                device,
            )
            for n, (a, b, device) in enumerate(
                ((0, 2, across), (0, 1, core), (2, 3, core))
            )
        ]

    def activate(c):
        cross_copy(c).wait_recv()
        first = 3 * quarter_head

        def to_hidden(rows):
            total = kept[c % 2, rows, first:] + cross_in[c, rows, first:].astype(f32)
            hid[c, rows, 0:quarter_ff] = (
                0.5 * total * (1.0 + lax.erf(total * (0.5**0.5)))
            ).astype(bf16)

        over_rows(seq, to_hidden)
        to_across, to_core, _ = share_copies(c, 0)
        to_across.start()
        to_core.start()
        for h in range(quarter_head // head):

            def of(t):
                cols = slice(t * quarter_head + h * head, t * quarter_head + (h + 1) * head)
                return kept[c % 2, :, cols] + cross_in[c, :, cols].astype(f32)

            query = layer_norm(of(0), query_gain[...]).astype(bf16)
            key = layer_norm(of(1), key_gain[...]).astype(bf16)
            value = of(2).astype(bf16)
            scores = lax.dot_general(
                query, key, (((1,), (1,)), ((), ())), preferred_element_type=f32
            ) * head ** (-0.5)
            raised = jnp.exp(scores)
            weights = (raised / jnp.sum(raised, axis=-1, keepdims=True)).astype(bf16)
            att[c, :, h * head : (h + 1) * head] = mul(weights, value).astype(bf16)
        to_across, to_core, _ = share_copies(c, 1)
        to_across.start()
        to_core.start()

    def forward(c):
        for which in range(2):
            from_across, _, onward = share_copies(c, which)
            from_across.wait_recv()
            onward.start()

    def branch_copy(p):
        c, b = p // 2, p % 2
        return remote(
            branch.at[c % 2, b, 0],
            branch_in.at[p % 4],
            branch_send.at[p],
            branch_recv.at[p],
            side,
        )

    def finish(c):
        for which, held, weight, copies in (
            (1, att, w_out, out_copies),
            (0, hid, w_down, down_copies),
        ):
            _, from_core, onward = share_copies(c, which)
            from_core.wait_recv()
            onward.wait_recv()
            if c == 0:
                for copy in copies:
                    copy.wait()
            b = 1 - which
            p = 2 * c + b
            if p >= 4:
                branch_copy(p - 4).wait_send()

            def one(s, carry):
                for n0 in range(0, slice_width, 256):
                    n1 = min(n0 + 256, slice_width)
                    branch[c % 2, b, s, :, n0:n1] = mul(
                        held[c], weight[s, :, n0:n1]
                    ).astype(bf16)

                @pl.when(s == 0)
                def _():
                    if p >= 4:
                        pl.semaphore_wait(branch_credit, 1)
                    branch_copy(p).start()

                return carry

            lax.fori_loop(0, 2, one, 0)

    from_low = jnp.logical_and(z <= g, z > 0)
    from_high = jnp.logical_and(z >= g, z < n_gx - 1)
    below, above = z < g, z > g

    def line_copies(p):
        c, b = p // 2, p % 2
        k = p % 4
        up = remote(
            line_out.at[k], line_low.at[k], line_send.at[p], low_recv.at[p], (g, j + sub)
        )
        down = remote(
            line_out.at[k],
            line_high.at[k],
            line_send.at[p],
            high_recv.at[p],
            (g, j - sub),
        )
        home = remote(
            line_out.at[k], final.at[b], line_send.at[p], final_recv.at[b], (c, j)
        )
        return up, down, home

    def leaves(p):
        return jnp.logical_not(jnp.logical_and(at_root, g == p // 2))

    def reduce(p):
        c, b = p // 2, p % 2
        k = p % 4
        up, down, home = line_copies(p)
        branch_copy(p).wait_recv()

        def begin(rows):
            running[rows] = branch[c % 2, b, 1, rows].astype(f32) + branch_in[
                k, rows
            ].astype(f32)

        over_rows(seq, begin)
        if p < 4:
            pl.semaphore_signal(
                branch_credit, inc=1, device_id=side, device_id_type=MESH
            )
        for here, copy, held, source in (
            (from_low, up, line_low, (g, j - sub)),
            (from_high, down, line_high, (g, j + sub)),
        ):

            @pl.when(here)
            def _():
                copy.wait_recv()

                def add(rows):
                    running[rows] = running[rows] + held[k, rows].astype(f32)

                over_rows(seq, add)
                if p < 4:
                    pl.semaphore_signal(
                        line_credit, inc=1, device_id=source, device_id_type=MESH
                    )

        if p >= 4:

            @pl.when(leaves(p - 4))
            def _():
                line_copies(p - 4)[0].wait_send()

            @pl.when(jnp.logical_not(at_root))
            def _():
                pl.semaphore_wait(line_credit, 1)

        def settle(rows):
            line_out[k, rows] = running[rows].astype(bf16)

        over_rows(seq, settle)

        @pl.when(below)
        def _():
            up.start()

        @pl.when(above)
        def _():
            down.start()

        @pl.when(at_root)
        def _():
            @pl.when(g == c)
            def _():
                final[b] = line_out[k]

            @pl.when(g != c)
            def _():
                home.start()

    gather(0)
    exchange(0)
    gather(1)
    exchange(1)
    gather(2)
    gather(3)
    activate(0)
    exchange(2)
    activate(1)
    forward(0)
    finish(0)
    exchange(3)
    activate(2)
    reduce(0)
    reduce(1)
    forward(1)
    finish(1)
    activate(3)
    reduce(2)
    reduce(3)
    forward(2)
    finish(2)
    forward(3)
    finish(3)
    for p in range(4, 8):
        reduce(p)

    for copy in keep_copies:
        copy.wait()

    @pl.when(jnp.logical_not(at_root))
    def _():
        for b in range(2):
            line_copies(b)[2].wait_recv()

    def last(rows):
        total = keeps[0, 0, rows].astype(f32) * final[0, rows].astype(f32)
        total = total + keeps[1, 0, rows].astype(f32) * final[1, rows].astype(f32)
        result[0, rows] = (tokens[0, rows].astype(f32) + total * keep_scale).astype(
            bf16
        )

    over_rows(seq, last)

    for copy in stat_copies:
        copy.wait_send()

    @pl.when(jnp.logical_not(at_root))
    def _():
        for copy in first_copies:
            copy.wait_send()

    for c in range(chunks):
        for p in range(GATHER_PIECES):
            down, up, beside = gather_copies(c, p)
            beside.wait_send()

            @pl.when(goes_up)
            def _():
                up.wait_send()

            @pl.when(goes_down)
            def _():
                down.wait_send()

        for which in range(2):
            for copy in share_copies(c, which):
                copy.wait_send()
    for half in range(2):
        part_copy(chunks - 1, half).wait_send()
    for c in range(chunks - 2, chunks):
        cross_copy(c).wait_send()
    for p in range(4, 8):
        branch_copy(p).wait_send()

        @pl.when(leaves(p))
        def _():
            line_copies(p)[0].wait_send()


def fused(
    tokens,
    norm_gain,
    qkv_weight,
    up_weight,
    query_gain,
    key_gain,
    out_weight,
    down_weight,
    attention_keep,
    feedforward_keep,
):
    n_gx, n_gy = lax.axis_size("gx"), lax.axis_size("gy")
    _, seq, slice_width = tokens.shape
    block_width, _, head_cols = qkv_weight.shape
    ff_cols = up_weight.shape[1]
    head = query_gain.shape[0]
    quarter_head, quarter_ff = head_cols // n_gx, ff_cols // n_gx
    quarter = 3 * quarter_head + quarter_ff
    chunks, pieces = n_gx, 2 * n_gx
    dma, vmem = pltpu.SemaphoreType.DMA, pltpu.VMEM
    scratch = [
        vmem((n_gx, block_width, quarter), bf16),
        vmem((2, ff_cols, slice_width), bf16),
        vmem((2, head_cols, slice_width), bf16),
        vmem((2, 1, seq, slice_width), jnp.int32),
        vmem((8, seq), f32),
        vmem((n_gy, 8, seq), f32),
        vmem((seq, slice_width), bf16),
        vmem((chunks, seq, block_width), bf16),
        vmem((n_gx, seq, quarter), bf16),
        vmem((2, 2, seq, quarter), bf16),
        vmem((2, seq, quarter), f32),
        vmem((2, seq, quarter), bf16),
        vmem((chunks, seq, quarter), bf16),
        vmem((chunks, seq, ff_cols), bf16),
        vmem((chunks, seq, head_cols), bf16),
        vmem((2, 2, 2, seq, slice_width), bf16),
        vmem((4, seq, slice_width), bf16),
        vmem((4, seq, slice_width), bf16),
        vmem((4, seq, slice_width), bf16),
        vmem((4, seq, slice_width), bf16),
        vmem((seq, slice_width), f32),
        vmem((2, seq, slice_width), bf16),
        dma((n_gx, 8)),
        dma((2, n_gx)),
        dma((2, n_gx)),
        dma((2,)),
        dma((n_gy,)),
        dma((n_gy,)),
        dma((GATHER_PIECES,)),
        dma((chunks, GATHER_PIECES)),
        dma((2, chunks, GATHER_PIECES)),
        dma((chunks, GATHER_PIECES)),
        dma((chunks, GATHER_PIECES)),
        dma((chunks, 2)),
        dma((chunks, 2)),
        dma((chunks,)),
        dma((chunks,)),
        dma((chunks, 2, 3)),
        dma((chunks, 2, 3)),
        dma((pieces,)),
        dma((pieces,)),
        dma((pieces,)),
        dma((pieces,)),
        dma((pieces,)),
        dma((2,)),
        pltpu.SemaphoreType.REGULAR,
        pltpu.SemaphoreType.REGULAR,
    ]
    in_vmem = pl.BlockSpec(memory_space=pltpu.VMEM)
    anywhere = pl.BlockSpec(memory_space=pl.ANY)
    return pl.pallas_call(
        functools.partial(block_kernel, n_gy),
        out_shape=jax.ShapeDtypeStruct(tokens.shape, bf16),
        in_specs=[in_vmem] * 4 + [anywhere] * 6,
        out_specs=in_vmem,
        scratch_shapes=scratch,
        compiler_params=pltpu.CompilerParams(
            collective_id=0, has_side_effects=True, vmem_limit_bytes=VMEM_LIMIT
        ),
    )(
        tokens,
        norm_gain.reshape(n_gy, 1, slice_width),
        query_gain.reshape(1, head),
        key_gain.reshape(1, head),
        jnp.transpose(qkv_weight, (1, 0, 2)),
        up_weight,
        out_weight,
        down_weight,
        attention_keep,
        feedforward_keep,
    )


def dispatch(*arrays):
    n_gx, n_gy = lax.axis_size("gx"), lax.axis_size("gy")
    images, seq, slice_width = arrays[0].shape
    head_cols, ff_cols = arrays[2].shape[2], arrays[3].shape[1]
    head = arrays[4].shape[0]
    fits = (
        n_gx == 4
        and n_gy == 2 * n_gx
        and images == 1
        and head == 128
        and head_cols % (n_gx * head) == 0
        and ff_cols % (n_gx * 128) == 0
        and slice_width % 128 == 0
        and seq % 128 == 0
    )
    return fused(*arrays) if fits else per_device(*arrays)


def solution(mesh):
    in_specs = (
        P("gx", None, "gy"),
        P(),
        P("gx", None, "gy"),
        P("gx", "gy"),
        P(),
        P(),
        P("gy", "gx"),
        P("gy", "gx"),
        P("gx", None, "gy"),
        P("gx", None, "gy"),
    )
    out_specs = P("gx", None, "gy")
    return jax.shard_map(
        dispatch, mesh=mesh, in_specs=in_specs, out_specs=out_specs, check_vma=False
    )
```

```python
import functools

import jax
import jax.numpy as jnp
from jax import lax
from jax.experimental import pallas as pl
from jax.experimental.pallas import tpu as pltpu
from jax.sharding import PartitionSpec as P

epsilon = 1e-06
keep_scale = 1.0 / 0.9
UP_CHUNKS = 2

f32 = jnp.float32
bf16 = jnp.bfloat16


def layer_norm(values, gain):
    center = values - jnp.mean(values, axis=-1, keepdims=True)
    variance = jnp.mean(center * center, axis=-1, keepdims=True)
    return center * lax.rsqrt(variance + epsilon) * gain


def head_norm(values, gain):
    row_count = values.shape[0]
    shaped = values.reshape(row_count, -1, gain.shape[0])
    return layer_norm(shaped, gain).reshape(row_count, -1)


def mul(left, right):
    return jnp.dot(left, right, preferred_element_type=f32)


def swap(values, bit, n_gx):
    return lax.ppermute(values, "gx", [(i, i ^ bit) for i in range(n_gx)])


def scatter_sum(odd_rows, even_rows, weight, n_gx):
    received = swap(mul(odd_rows, weight).astype(bf16), 1, n_gx)
    total = mul(even_rows, weight).astype(bf16).astype(f32) + received.astype(f32)
    bit, width = 2, weight.shape[1]
    own_rows = 2 * odd_rows.shape[0] // n_gx
    while bit < n_gx:
        pairs = total.reshape(-1, 2, own_rows, width)
        received = swap(pairs[:, 1].astype(bf16), bit, n_gx)
        total = pairs[:, 0] + received.astype(f32)
        bit *= 2
    return total.reshape(own_rows, width)


def gather_pair(own, n_gx):
    held, bit = own, n_gx // 2
    while bit > 1:
        held = jnp.concatenate([held, swap(held, bit, n_gx)], axis=0)
        bit //= 2
    return held, swap(held, 1, n_gx)


def gather_order(n_gx):
    order, bit = [0], n_gx // 2
    while bit >= 1:
        order = order + [p ^ bit for p in order]
        bit //= 2
    return order


def ring_place(index, count):
    return jnp.where(index % 2 == 0, index // 2, count - 1 - index // 2)


def ring_gather(own, ring, place):
    n = len(ring)
    ahead = [(ring[r], ring[(r + 1) % n]) for r in range(n)]
    back = [(b, a) for a, b in ahead]
    forward, backward = [own], [own]
    for step in range(n // 2 - 1):
        forward.append(lax.ppermute(forward[-1], "gy", ahead))
        backward.append(lax.ppermute(backward[-1], "gy", back))
    half = own.shape[0] // 2
    far = jnp.concatenate(
        [
            lax.ppermute(forward[-1][:half], "gy", ahead),
            lax.ppermute(backward[-1][half:], "gy", back),
        ],
        axis=0,
    )
    return jnp.stack(forward + [far] + backward[:0:-1])


def ring_scatter(partial, ring, place):
    n = len(ring)
    half = partial.shape[1] // 2
    ahead = [(ring[r], ring[(r + 1) % n]) for r in range(n)]
    back = [(b, a) for a, b in ahead]

    def block(index, start):
        index = lax.rem(index + 2 * n, n)
        return lax.dynamic_slice(
            partial, (index, start, 0), (1, half, partial.shape[2])
        )[0]

    up, down = block(place - 1, 0), block(place + 1, half)
    for step in range(n - 1):
        came_up = lax.ppermute(up, "gy", ahead)
        came_down = lax.ppermute(down, "gy", back)
        up = came_up.astype(f32) + block(place - 2 - step, 0).astype(f32)
        down = came_down.astype(f32) + block(place + 2 + step, half).astype(f32)
        up, down = up.astype(bf16), down.astype(bf16)
    return jnp.concatenate([up, down], axis=0)


def per_device(
    tokens,
    norm_gain,
    qkv_weight,
    up_weight,
    query_gain,
    key_gain,
    out_weight,
    down_weight,
    attention_keep,
    feedforward_keep,
):
    n_gx, n_gy = lax.axis_size("gx"), lax.axis_size("gy")
    sub = n_gy // n_gx
    me = lax.axis_index("gx")
    ring = list(range(0, n_gy, 2)) + list(range(1, n_gy, 2))[::-1]
    place = ring_place(lax.axis_index("gy"), n_gy)
    images, seq_len, slice_width = tokens.shape
    own_rows = images * seq_len
    block_width = qkv_weight.shape[0]
    head_cols = qkv_weight.shape[2]
    head_size = query_gain.shape[0]

    flat = tokens.reshape(own_rows, slice_width)
    turned = lax.ppermute(
        flat,
        ("gx", "gy"),
        [
            (i * n_gy + k * sub + s, k * n_gy + i * sub + s)
            for i in range(n_gx)
            for k in range(n_gx)
            for s in range(sub)
        ],
    )
    gathered = ring_gather(turned, ring, place)

    wide = flat.astype(f32)
    mean = jnp.mean(wide, axis=1)
    squares = jnp.sum((wide - mean[:, None]) ** 2, axis=1)
    count, bit = slice_width, 1
    while bit < n_gy:
        pairs = [(i, i ^ bit) for i in range(n_gy)]
        other = lax.ppermute(jnp.stack([mean, squares]), "gy", pairs)
        squares = squares + other[1] + (0.5 * count) * (mean - other[0]) ** 2
        mean = 0.5 * (mean + other[0])
        count, bit = 2 * count, 2 * bit
    stats = jnp.stack([mean, lax.rsqrt(squares / count + epsilon)])[None]
    bit = 1
    while bit < n_gx:
        stats = jnp.concatenate([stats, swap(stats, bit, n_gx)], axis=0)
        bit *= 2
    gain = lax.dynamic_slice_in_dim(norm_gain, me * block_width, block_width, 0)

    def normed_rows(position):
        image = me ^ position
        rows = jnp.concatenate(
            [
                lax.dynamic_index_in_dim(
                    gathered,
                    lax.rem(place - ring_place(image * sub + s, n_gy) + n_gy, n_gy),
                    0,
                    keepdims=False,
                )
                for s in range(sub)
            ],
            axis=1,
        ).astype(f32)
        row_mean, row_scale = stats[position, 0], stats[position, 1]
        return ((rows - row_mean[:, None]) * row_scale[:, None] * gain).astype(bf16)

    odd_rows = jnp.concatenate([normed_rows(p) for p in range(1, n_gx, 2)], axis=0)
    even_rows = jnp.concatenate([normed_rows(p) for p in range(0, n_gx, 2)], axis=0)

    qkv_flat = qkv_weight.reshape(block_width, 3 * head_cols)
    united = scatter_sum(odd_rows, even_rows, qkv_flat, n_gx)
    up_cols = up_weight.shape[1] // UP_CHUNKS
    hidden = []
    for c in range(UP_CHUNKS):
        total = scatter_sum(
            odd_rows, even_rows, up_weight[:, c * up_cols : (c + 1) * up_cols], n_gx
        )
        hidden.append(jax.nn.gelu(total, approximate=False).astype(bf16))

    queries = head_norm(united[:, :head_cols], query_gain).astype(bf16)
    keys = head_norm(united[:, head_cols : 2 * head_cols], key_gain).astype(bf16)
    values = united[:, 2 * head_cols :].astype(bf16)
    query_grid = queries.reshape(images, seq_len, -1, head_size)
    key_grid = keys.reshape(images, seq_len, -1, head_size)
    value_grid = values.reshape(images, seq_len, -1, head_size)
    scores = jnp.einsum(
        "bshd,bthd->bhst", query_grid, key_grid, preferred_element_type=f32
    ) * head_size ** (-0.5)
    raised = jnp.exp(scores)
    weights = (raised / jnp.sum(raised, axis=-1, keepdims=True)).astype(bf16)
    attended = jnp.einsum("bhst,bthd->bshd", weights, value_grid, preferred_element_type=f32)
    attended = attended.astype(bf16).reshape(own_rows, head_cols)

    order = gather_order(n_gx)
    def home(devices):
        return [
            (
                k * n_gy + devices[s * n_gx + q],
                (k ^ order[q]) * n_gy + k * sub + s,
            )
            for k in range(n_gx)
            for s in range(sub)
            for q in range(n_gx)
        ]

    def columns(weight, s):
        return weight[:, s * slice_width : (s + 1) * slice_width]

    attended_halves = gather_pair(attended, n_gx)
    attention_out = lax.psum_scatter(
        jnp.concatenate(
            [
                mul(rows, columns(out_weight, s)).astype(bf16)
                for s in range(sub)
                for rows in attended_halves
            ],
            axis=0,
        ),
        "gy",
        scatter_dimension=0,
        tiled=True,
    )
    attention_out = lax.ppermute(attention_out, ("gx", "gy"), home(range(n_gy))).astype(f32)
    hidden_halves = [gather_pair(part, n_gx) for part in hidden]
    pieces = []
    for s in range(sub):
        for half in range(2):
            total = 0.0
            for c in range(UP_CHUNKS):
                weight = down_weight[c * up_cols : (c + 1) * up_cols]
                total = total + mul(hidden_halves[c][half], columns(weight, s))
            pieces.append(total.astype(bf16))
    partial = jnp.concatenate(pieces, axis=0).reshape(n_gy, own_rows, slice_width)
    feedforward_out = ring_scatter(partial, ring, place)
    feedforward_out = lax.ppermute(feedforward_out, ("gx", "gy"), home(ring)).astype(f32)

    shape = tokens.shape
    branches = attention_keep.astype(f32) * attention_out.reshape(
        shape
    ) + feedforward_keep.astype(f32) * feedforward_out.reshape(shape)
    return (tokens.astype(f32) + branches * keep_scale).astype(bf16)


MESH = pl.DeviceIdType.MESH
VMEM_LIMIT = 67043328
GATHER_PIECES = 4
ROW_STEP = 64
FIRST_SECTIONS = 1


def flip(index, mask):
    for bit in (1, 2):
        if mask & bit:
            index = index + bit - 2 * bit * ((index // bit) % 2)
    return index


SCHEDULE = (
    "mark0", "relay0", "relay1", "relay2/root", "relay3/root", "gather0", "exchange0",
    "relay2/mid", "exchange1", "masks0/root", "relay3/mid", "activate0",
    "masks1/root", "gather3", "exchange2", "activate1", "masks0/near", "forward0", "finish0",
    "masks1/near", "reduce0/0", "activate2", "exchange3", "masks0/far", "reduce1/0",
    "reduce0/1", "forward1", "finish1", "masks1/far", "reduce1/1", "reduce0/2", "forward2",
    "finish2", "reduce2/0", "reduce3/0", "reduce1/2", "activate3", "reduce2/1", "reduce0/3",
    "reduce1/3", "reduce4/0", "reduce3/1", "forward3", "masks0/end", "masks1/end",
    "finish3", "reduce5/0", "close3", "reduce2/2", "reduce3/2", "reduce2/3", "reduce3/3", "reduce4/late",
    "reduce5/late", "reduce6", "reduce7",
)


def schedule():
    for word in SCHEDULE:
        name, _, role = word.partition("/")
        yield name[:-1], int(name[-1]), role


def remote(src, dst, send_sem, recv_sem, device):
    return pltpu.make_async_remote_copy(
        src_ref=src,
        dst_ref=dst,
        send_sem=send_sem,
        recv_sem=recv_sem,
        device_id=device,
        device_id_type=MESH,
    )


scope = jax.named_scope


def over_rows(count, body):
    def step(i, carry):
        body(pl.ds(pl.multiple_of(i * ROW_STEP, ROW_STEP), ROW_STEP))
        return carry

    lax.fori_loop(0, count // ROW_STEP, step, 0)


def aligned(start, size):
    return pl.ds(pl.multiple_of(start, size), size)


def block_kernel(
    n_gy,
    tokens,
    gain,
    query_gain,
    key_gain,
    qkv_hbm,
    up_hbm,
    out_hbm,
    down_hbm,
    attention_keep,
    feedforward_keep,
    result,
    *scratch,
):
    (
        w_in,
        w_down,
        w_out,
        keeps,
        stat_own,
        stat_all,
        normed,
        rows_in,
        part,
        part_in,
        kept,
        cross,
        cross_in,
        hid,
        att,
        branch,
        merged,
        branch_in,
        line_out,
        line_low,
        line_high,
        final,
        mask_own,
        mask_in,
        in_sem,
        down_sem,
        out_sem,
        keep_sem,
        stat_send,
        stat_recv,
        first_send,
        gather_recv,
        gather_send,
        side_send,
        side_recv,
        part_send,
        part_recv,
        cross_send,
        cross_recv,
        share_send,
        share_recv,
        branch_send,
        branch_recv,
        line_send,
        low_recv,
        high_recv,
        final_recv,
        mask_first,
        mask_recv,
        mask_send,
        mask_side,
        line_credit,
        turn,
    ) = scratch
    n_gx = 4
    sub = n_gy // n_gx
    g, j = lax.axis_index("gx"), lax.axis_index("gy")
    z, x = j // sub, j % sub
    core, across, side = (flip(g, 1), j), (flip(g, 2), j), (g, j + 1 - 2 * x)
    seq, slice_width = normed.shape
    features = n_gy * slice_width
    head = query_gain.shape[1]
    quarter_head, quarter_ff = att.shape[2] // n_gx, hid.shape[2] // n_gx
    quarter = part.shape[2]
    chunks = n_gx
    step_rows = seq // GATHER_PIECES
    own_cols, side_cols = pl.ds(0, slice_width), pl.ds(slice_width, slice_width)

    relative = (3, 2, 1, 0)
    in_copies, down_copies, out_copies = [], [], []
    for q, r in enumerate(relative):
        k = flip(g, r)
        copies = []
        for h in range(2):
            from_rows = aligned(slice_width * (x if h == 0 else 1 - x), slice_width)
            to_rows = pl.ds(h * slice_width, slice_width)
            for t in range(3):
                copies.append(
                    (
                        qkv_hbm.at[t, from_rows, aligned(k * quarter_head, quarter_head)],
                        w_in.at[q, to_rows, pl.ds(t * quarter_head, quarter_head)],
                    )
                )
            copies.append(
                (
                    up_hbm.at[from_rows, aligned(k * quarter_ff, quarter_ff)],
                    w_in.at[q, to_rows, pl.ds(3 * quarter_head, quarter_ff)],
                )
            )
        in_copies.append(
            [
                pltpu.make_async_copy(a, b, in_sem.at[q, n])
                for n, (a, b) in enumerate(copies)
            ]
        )
    for s in range(2):
        from_cols = aligned(slice_width * (1 - x if s == 0 else x), slice_width)
        for r in range(n_gx):
            k = flip(g, r)
            down_copies.append(
                pltpu.make_async_copy(
                    down_hbm.at[aligned(k * quarter_ff, quarter_ff), from_cols],
                    w_down.at[s, pl.ds(r * quarter_ff, quarter_ff)],
                    down_sem.at[s, r],
                )
            )
            out_copies.append(
                pltpu.make_async_copy(
                    out_hbm.at[aligned(k * quarter_head, quarter_head), from_cols],
                    w_out.at[s, pl.ds(r * quarter_head, quarter_head)],
                    out_sem.at[s, r],
                )
            )
    keep_copies = [
        pltpu.make_async_copy(attention_keep, keeps.at[0], keep_sem.at[0]),
        pltpu.make_async_copy(feedforward_keep, keeps.at[1], keep_sem.at[1]),
    ]
    mark_scope = scope('begin')
    mark_scope.__enter__()
    for copies in in_copies:
        for copy in copies:
            copy.start()
    for copy in down_copies + out_copies + keep_copies:
        copy.start()

    barrier = pltpu.get_barrier_semaphore()
    for r in range(1, n_gx):
        pl.semaphore_signal(
            barrier, inc=1, device_id=(flip(g, r), j), device_id_type=MESH
        )
    for d in range(1, n_gy):
        pl.semaphore_signal(
            barrier, inc=1, device_id=(g, (j + d) % n_gy), device_id_type=MESH
        )

    mark_scope.__exit__(None, None, None)
    mark_scope = scope('moments')
    mark_scope.__enter__()
    wide = tokens[0].astype(f32)
    mean = jnp.mean(wide, axis=1, keepdims=True)
    squares = jnp.sum((wide - mean) ** 2, axis=1, keepdims=True)
    mean_row = jnp.transpose(jnp.broadcast_to(mean, (seq, 128)))[:8]
    squares_row = jnp.transpose(jnp.broadcast_to(squares, (seq, 128)))[:8]
    top = lax.broadcasted_iota(jnp.int32, (8, seq), 0) == 0
    stats = jnp.where(top, mean_row, squares_row)
    stat_own[...] = stats
    stat_all[0] = stats
    mark_scope.__exit__(None, None, None)
    mark_scope = scope('barrier')
    mark_scope.__enter__()
    pl.semaphore_wait(barrier, n_gx + n_gy - 2)
    mark_scope.__exit__(None, None, None)
    mark_scope = scope('swap')
    mark_scope.__enter__()
    stat_copies = [
        remote(
            stat_own,
            stat_all.at[d],
            stat_send.at[d],
            stat_recv.at[d],
            (g, (j + d) % n_gy),
        )
        for d in range(1, n_gy)
    ]
    for copy in stat_copies:
        copy.start()
    for copy in stat_copies:
        copy.wait_recv()
    mark_scope.__exit__(None, None, None)
    mark_scope = scope('norm')
    mark_scope.__enter__()
    means = [stat_all[d, 0:1] for d in range(n_gy)]
    total_mean = sum(means) * (1.0 / n_gy)
    spread = sum((m - total_mean) ** 2 for m in means) * float(slice_width)
    spread = spread + sum(stat_all[d, 1:2] for d in range(n_gy))
    scale = lax.rsqrt(spread * (1.0 / features) + epsilon)
    mean_col = jnp.transpose(jnp.broadcast_to(total_mean, (128, seq)))
    scale_col = jnp.transpose(jnp.broadcast_to(scale, (128, seq)))
    for c0 in range(0, slice_width, 128):
        cols = slice(c0, c0 + 128)
        centre = tokens[0, :, cols].astype(f32) - mean_col
        normed[:, cols] = (centre * scale_col * gain[j, :, cols]).astype(bf16)

    at_root = g == z
    first_copies = [
        remote(
            normed.at[pl.ds(p * step_rows, step_rows)],
            rows_in.at[g, pl.ds(p * step_rows, step_rows), own_cols],
            first_send.at[p],
            gather_recv.at[g, p],
            (z, j),
        )
        for p in range(GATHER_PIECES)
    ]

    @pl.when(at_root)
    def _():
        rows_in[g, :, own_cols] = normed[...]

    mark_scope.__exit__(None, None, None)
    @pl.when(g % 2 == 1)
    def _():
        pl.semaphore_wait(turn, 1)

    @pl.when(jnp.logical_not(at_root))
    def _():
        for copy in first_copies:
            copy.start()

    @pl.when(g % 2 == 0)
    def _():
        @pl.when(jnp.logical_not(at_root))
        def _():
            for copy in first_copies:
                copy.wait_send()

        pl.semaphore_signal(turn, inc=1, device_id=core, device_id_type=MESH)

    join = chunks - 1
    half_rows = seq // 2

    def mask_ref(i):
        return mask_in.at[i // 4, i // 2 % 2, pl.ds(i % 2 * half_rows, half_rows)]

    def mask_first_copy(i):
        return remote(
            mask_own.at[i // 2, pl.ds(i % 2 * half_rows, half_rows)],
            mask_ref(i),
            mask_first.at[i],
            mask_recv.at[i],
            (z, j),
        )

    def mark(_):
        @pl.when(g >= join)
        def _():
            for b in range(2):
                keep_copies[b].wait()

                def to_mask(rows):
                    mask_own[b, rows] = keeps[b, 0, rows].astype(f32).astype(bf16)

                over_rows(seq, to_mask)

            @pl.when(at_root)
            def _():
                mask_in[0] = mask_own[...]

            @pl.when(jnp.logical_not(at_root))
            def _():
                for i in range(4):
                    mask_first_copy(i).start()

    goes_down = jnp.logical_and(z <= g, z > 0)
    goes_up = jnp.logical_and(z >= g, z < n_gx - 1)
    duty = jnp.logical_or(goes_down, goes_up)

    def mask_copies(i):
        own = mask_ref(i)
        down = remote(own, own, mask_send.at[0, i], mask_recv.at[i], (g, j - sub))
        up = remote(own, own, mask_send.at[1, i], mask_recv.at[i], (g, j + sub))
        return down, up

    def mask_beside(i):
        return remote(
            mask_ref(i), mask_ref(4 + i), mask_side.at[i], mask_recv.at[4 + i], side
        )

    def masks(s):
        for i in range(4 * s, 4 * s + 4):
            down, up = mask_copies(i)
            if s == 0:

                @pl.when(jnp.logical_not(jnp.logical_and(at_root, g == join)))
                def _():
                    up.wait_recv()

                @pl.when(at_root)
                def _():
                    mask_beside(i).start()

            else:
                up.wait_recv()

            @pl.when(goes_up)
            def _():
                up.start()

            @pl.when(goes_down)
            def _():
                down.start()

    def gather_ref(c, p, cols):
        return rows_in.at[c, pl.ds(p * step_rows, step_rows), cols]

    def gather_copies(c, p):
        own = gather_ref(c, p, own_cols)
        down = remote(
            own, own, gather_send.at[0, c, p], gather_recv.at[c, p], (g, j - sub)
        )
        up = remote(
            own, own, gather_send.at[1, c, p], gather_recv.at[c, p], (g, j + sub)
        )
        beside = remote(
            own,
            gather_ref(c, p, side_cols),
            side_send.at[c, p],
            side_recv.at[c, p],
            side,
        )
        return down, up, beside

    def gather(c, pieces=range(GATHER_PIECES)):
        for p in pieces:
            down, up, beside = gather_copies(c, p)

            @pl.when(jnp.logical_not(jnp.logical_and(at_root, g == c)))
            def _():
                up.wait_recv()

            @pl.when(goes_up)
            def _():
                up.start()

            @pl.when(goes_down)
            def _():
                down.start()

            beside.start()

    def gathered(c, pieces):
        for p in pieces:
            gather_copies(c, p)[2].wait_recv()

    def sections(c):
        count = FIRST_SECTIONS if c == 0 else 1
        return [
            (sec, slice(sec * seq // count, (sec + 1) * seq // count))
            for sec in range(count)
        ]

    def part_copy(c, half, section):
        sec, rows = section
        return remote(
            part.at[2 * half, rows],
            part_in.at[c % 2, half, rows],
            part_send.at[c, half, sec],
            part_recv.at[c, half, sec],
            core,
        )

    def cross_copy(c, section):
        sec, rows = section
        return remote(
            cross.at[c % 2, rows],
            cross_in.at[c, rows],
            cross_send.at[c, sec],
            cross_recv.at[c, sec],
            across,
        )

    def project(c, half, section):
        rows = section[1]
        if c == 0 and section[0] == 0:
            for copy in in_copies[2 * half] + in_copies[2 * half + 1]:
                copy.wait()
        if c > 0:
            for earlier in sections(c - 1):
                part_copy(c - 1, half, earlier).wait_send()

        def one(i, carry):
            q = 2 * half + i
            for n0 in range(0, quarter, 256):
                n1 = min(n0 + 256, quarter)
                part[q, rows, n0:n1] = mul(
                    rows_in[c, rows], w_in[q, :, n0:n1]
                ).astype(bf16)

            @pl.when(i == 0)
            def _():
                part_copy(c, half, section).start()

            return carry

        lax.fori_loop(0, 2, one, 0)

    def exchange(c):
        if c >= slots:
            for unit in range(3):
                share_copies(c - slots, unit)[2].wait_send()
        if c >= 2:
            for earlier in sections(c - 2):
                cross_copy(c - 2, earlier).wait_send()
        for section in sections(c):
            rows = section[1]
            pieces = range(rows.start // step_rows, rows.stop // step_rows)
            gathered(c, pieces)
            project(c, 0, section)
            part_copy(c, 0, section).wait_recv()

            def to_cross(step):
                here = pl.ds(rows.start + step.start, ROW_STEP)
                total = part[1, here].astype(f32) + part_in[c % 2, 0, here].astype(f32)
                cross[c % 2, here] = total.astype(bf16)

            over_rows(rows.stop - rows.start, to_cross)
            cross_copy(c, section).start()
            half_pieces = GATHER_PIECES // 2
            if c < 2:
                early = range(half_pieces)
                pl.when(jnp.logical_not(duty))(functools.partial(gather, c + 1, early))
            project(c, 1, section)
            if c < 2:
                late = range(half_pieces, GATHER_PIECES)
                pl.when(jnp.logical_not(duty))(functools.partial(gather, c + 1, late))
            part_copy(c, 1, section).wait_recv()

            def to_kept(step):
                here = pl.ds(rows.start + step.start, ROW_STEP)
                kept[c % 2, here] = part[3, here].astype(f32) + part_in[
                    c % 2, 1, here
                ].astype(f32)

            over_rows(rows.stop - rows.start, to_kept)

    slots = hid.shape[0]
    half_rows = seq // 2

    def half_of(h):
        return slice(h * half_rows, (h + 1) * half_rows)

    def share_copies(c, unit):
        held, width = (hid, quarter_ff) if unit < 2 else (att, quarter_head)
        rows = half_of(unit) if unit < 2 else slice(0, seq)

        def slot(r):
            return held.at[c % slots, rows, pl.ds(r * width, width)]

        return [
            remote(
                slot(a),
                slot(b),
                share_send.at[c, unit, n],
                share_recv.at[c, unit, n],
                device,
            )
            for n, (a, b, device) in enumerate(
                ((0, 2, across), (0, 1, core), (2, 3, core))
            )
        ]

    def share(c, unit):
        to_across, to_core, _ = share_copies(c, unit)
        to_across.start()
        to_core.start()

    def activate(c):
        if c >= slots:
            for unit in range(3):
                for copy in share_copies(c - slots, unit)[:2]:
                    copy.wait_send()
        for section in sections(c):
            cross_copy(c, section).wait_recv()
        order = (2, 0, 1) if c >= join else (0, 1, 2)
        for unit in order:
            if unit == 2:
                attend(c)
            else:
                activate_rows(c, unit * half_rows)
            share(c, unit)

    def activate_rows(c, offset):
        first = 3 * quarter_head

        def to_hidden(step):
            rows = pl.ds(offset + step.start, ROW_STEP)
            total = kept[c % 2, rows, first:] + cross_in[c, rows, first:].astype(f32)
            hid[c % slots, rows, 0:quarter_ff] = (
                0.5 * total * (1.0 + lax.erf(total * (0.5**0.5)))
            ).astype(bf16)

        over_rows(half_rows, to_hidden)

    def attend(c):
        for h in range(quarter_head // head):

            def of(t):
                cols = slice(t * quarter_head + h * head, t * quarter_head + (h + 1) * head)
                return kept[c % 2, :, cols] + cross_in[c, :, cols].astype(f32)

            query = layer_norm(of(0), query_gain[...]).astype(bf16)
            key = layer_norm(of(1), key_gain[...]).astype(bf16)
            value = of(2).astype(bf16)
            scores = lax.dot_general(
                query, key, (((1,), (1,)), ((), ())), preferred_element_type=f32
            ) * head ** (-0.5)
            raised = jnp.exp(scores)
            weights = (raised / jnp.sum(raised, axis=-1, keepdims=True)).astype(bf16)
            att[c % slots, :, h * head : (h + 1) * head] = mul(weights, value).astype(
                bf16
            )

    def onward(c, unit):
        from_across, _, to_core = share_copies(c, unit)
        from_across.wait_recv()
        to_core.start()

    def forward(c):
        for unit in (2, 0) if c >= join else (0, 1, 2):
            onward(c, unit)

    quarter_rows = seq // 4

    def piece_rows(p):
        if p // 4 < join:
            return slice(p % 2 * half_rows, (p % 2 + 1) * half_rows)
        return slice(p % 4 * quarter_rows, (p % 4 + 1) * quarter_rows)

    def piece_slot(p):
        return p // 2 if p // 4 < join else 2 * join

    def line_slot(p):
        return p // 2 % 4

    def line_rows(p):
        rows = piece_rows(p)
        start = p % 2 * half_rows
        return slice(start, start + rows.stop - rows.start)

    def branch_ref(p, s):
        c, b, rows = p // 4, p // 2 % 2, piece_rows(p)
        return branch.at[c, b, s, rows] if c < join else merged.at[s, rows]

    def branch_copy(p):
        return remote(
            branch_ref(p, 0),
            branch_in.at[piece_slot(p), piece_rows(p)],
            branch_send.at[p],
            branch_recv.at[p],
            side,
        )

    def shares_arrive(c, unit):
        for copy in share_copies(c, unit)[1:]:
            copy.wait_recv()
        if c == 0 and unit > 0:
            for copy in (down_copies, out_copies)[unit - 1]:
                copy.wait()

    def finish(c):
        if c >= join:
            finish_joined(c, 0)
            onward(c, 1)
            return
        for b, held, weight in ((0, att, w_out), (1, hid, w_down)):
            for unit in (2,) if b == 0 else (0, 1):
                shares_arrive(c, unit)

            def one(s, carry):
                for n0 in range(0, slice_width, 256):
                    n1 = min(n0 + 256, slice_width)
                    branch[c, b, s, :, n0:n1] = mul(
                        held[c % slots], weight[s, :, n0:n1]
                    ).astype(bf16)

                @pl.when(s == 0)
                def _():
                    for h in range(2):
                        branch_copy(4 * c + 2 * b + h).start()

                return carry

            lax.fori_loop(0, 2, one, 0)

    def finish_joined(c, h):
        if h == 0:
            shares_arrive(c, 2)
        shares_arrive(c, h)
        rows = half_of(h)

        def one(s, carry):
            for n0 in range(0, slice_width, 256):
                cols = slice(n0, min(n0 + 256, slice_width))
                keep_att = mask_in[1 - s, 0, rows, cols].astype(f32)
                keep_ff = mask_in[1 - s, 1, rows, cols].astype(f32)
                total = keep_att * mul(att[c % slots, rows], w_out[s, :, cols])
                total = total + keep_ff * mul(hid[c % slots, rows], w_down[s, :, cols])
                merged[s, rows, cols] = total.astype(bf16)

            @pl.when(s == 0)
            def _():
                for i in range(2):
                    branch_copy(4 * c + 2 * h + i).start()

            return carry

        lax.fori_loop(0, 2, one, 0)

    def close(c):
        finish_joined(c, 1)

    from_low = jnp.logical_and(z <= g, z > 0)
    from_high = jnp.logical_and(z >= g, z < n_gx - 1)
    below, above = z < g, z > g

    def line_copies(p):
        c = p // 4
        k, rows, held = line_slot(p), piece_rows(p), line_rows(p)
        own = line_out.at[k, held]
        up = remote(
            own, line_low.at[k, held], line_send.at[p], low_recv.at[p], (g, j + sub)
        )
        down = remote(
            own, line_high.at[k, held], line_send.at[p], high_recv.at[p], (g, j - sub)
        )
        landing = final.at[p // 2 % 2 if c < join else 0, rows]
        home = remote(own, landing, line_send.at[p], final_recv.at[p % 4], (c, j))
        return up, down, home

    def leaves(p):
        return jnp.logical_not(jnp.logical_and(at_root, g == p // 4))

    def reduce(n):
        for p in (2 * n, 2 * n + 1):
            reduce_piece(p)

    def reduce_piece(p):
        c = p // 4
        k, rows = line_slot(p), piece_rows(p)
        count, offset = rows.stop - rows.start, rows.start
        shift = line_rows(p).start
        up, down, home = line_copies(p)
        branch_copy(p).wait_recv()

        @pl.when(from_low)
        def _():
            up.wait_recv()

        @pl.when(from_high)
        def _():
            down.wait_recv()

        if p >= 8:

            @pl.when(leaves(p - 8))
            def _():
                line_copies(p - 8)[0].wait_send()

            @pl.when(jnp.logical_not(at_root))
            def _():
                pl.semaphore_wait(line_credit, 1)

        def total_rows(step):
            total = branch_ref(p, 1)[step].astype(f32) + branch_in[
                piece_slot(p), pl.ds(offset + step.start, ROW_STEP)
            ].astype(f32)
            low = line_low[k, pl.ds(shift + step.start, ROW_STEP)].astype(f32)
            high = line_high[k, pl.ds(shift + step.start, ROW_STEP)].astype(f32)
            total = total + jnp.where(from_low, low, 0.0)
            total = total + jnp.where(from_high, high, 0.0)
            line_out[k, pl.ds(shift + step.start, ROW_STEP)] = total.astype(bf16)

        over_rows(count, total_rows)
        if p < 8:
            for here, source in ((from_low, j - sub), (from_high, j + sub)):

                @pl.when(here)
                def _():
                    pl.semaphore_signal(
                        line_credit, inc=1, device_id=(g, source), device_id_type=MESH
                    )

        @pl.when(below)
        def _():
            up.start()

        @pl.when(above)
        def _():
            down.start()

        @pl.when(at_root)
        def _():
            @pl.when(g == c)
            def _():
                final[p // 2 % 2 if c < join else 0, rows] = line_out[k, line_rows(p)]

            @pl.when(g != c)
            def _():
                home.start()

    steps = dict(
        relay=gather,
        gather=gather,
        masks=masks,
        mark=mark,
        exchange=exchange,
        activate=activate,
        forward=forward,
        finish=finish,
        close=close,
        reduce=reduce,
    )
    hops = jnp.where(at_root, 3, jnp.where(below, z, n_gx - 1 - z))
    roles = {
        "relay": duty,
        "gather": jnp.logical_not(duty),
        "root": at_root,
        "mid": jnp.logical_and(duty, jnp.logical_not(at_root)),
        "near": jnp.logical_and(duty, jnp.abs(z - g) == 1),
        "far": jnp.logical_and(duty, jnp.abs(z - g) > 1),
        "end": jnp.logical_not(duty),
        "late": hops > 0,
    }
    for d in range(n_gx):
        roles[str(d)] = hops == d
    for act, c, role in schedule():
        with scope(f"{act}{c}"):
            step = functools.partial(steps[act], c)
            if role or act in ("relay", "gather"):
                pl.when(roles[role or act])(step)
            else:
                step()

    def arrive(p):
        @pl.when(jnp.logical_not(at_root))
        def _():
            line_copies(p)[2].wait_recv()

    @pl.when(g < join)
    def _():
        for b in range(2):
            keep_copies[b].wait()
        for p in range(4):
            arrive(p)

        def last(rows):
            total = keeps[0, 0, rows].astype(f32) * final[0, rows].astype(f32)
            total = total + keeps[1, 0, rows].astype(f32) * final[1, rows].astype(f32)
            result[0, rows] = (
                tokens[0, rows].astype(f32) + total * keep_scale
            ).astype(bf16)

        over_rows(seq, last)

    @pl.when(g >= join)
    def _():
        for p in range(4):
            arrive(4 * join + p)

        def last(rows):
            total = final[0, rows].astype(f32)
            result[0, rows] = (
                tokens[0, rows].astype(f32) + total * keep_scale
            ).astype(bf16)

        over_rows(seq, last)

        @pl.when(jnp.logical_not(at_root))
        def _():
            for i in range(4):
                mask_first_copy(i).wait_send()

    @pl.when(at_root)
    def _():
        for i in range(4):
            mask_beside(i).wait_send()

    for i in range(8):
        down, up = mask_copies(i)

        @pl.when(goes_up)
        def _():
            up.wait_send()

        @pl.when(goes_down)
        def _():
            down.wait_send()

    for copy in stat_copies:
        copy.wait_send()

    @pl.when(jnp.logical_and(jnp.logical_not(at_root), g % 2 == 1))
    def _():
        for copy in first_copies:
            copy.wait_send()

    for c in range(chunks):
        for p in range(GATHER_PIECES):
            down, up, beside = gather_copies(c, p)
            beside.wait_send()

            @pl.when(goes_up)
            def _():
                up.wait_send()

            @pl.when(goes_down)
            def _():
                down.wait_send()

        for unit in range(3) if c >= chunks - slots else []:
            for copy in share_copies(c, unit):
                copy.wait_send()
    for half in range(2):
        for section in sections(chunks - 1):
            part_copy(chunks - 1, half, section).wait_send()
    for c in range(chunks - 2, chunks):
        for section in sections(c):
            cross_copy(c, section).wait_send()
    for p in range(8):
        branch_copy(p).wait_send()
    for p in range(8, 16):
        branch_copy(p).wait_send()

        @pl.when(leaves(p))
        def _():
            line_copies(p)[0].wait_send()


def fused(
    tokens,
    norm_gain,
    qkv_weight,
    up_weight,
    query_gain,
    key_gain,
    out_weight,
    down_weight,
    attention_keep,
    feedforward_keep,
):
    n_gx, n_gy = lax.axis_size("gx"), lax.axis_size("gy")
    _, seq, slice_width = tokens.shape
    block_width, _, head_cols = qkv_weight.shape
    ff_cols = up_weight.shape[1]
    head = query_gain.shape[0]
    quarter_head, quarter_ff = head_cols // n_gx, ff_cols // n_gx
    quarter = 3 * quarter_head + quarter_ff
    chunks, pieces = n_gx, 4 * n_gx
    dma, vmem = pltpu.SemaphoreType.DMA, pltpu.VMEM
    scratch = [
        vmem((n_gx, block_width, quarter), bf16),
        vmem((2, ff_cols, slice_width), bf16),
        vmem((2, head_cols, slice_width), bf16),
        vmem((2, 1, seq, slice_width), jnp.int32),
        vmem((8, seq), f32),
        vmem((n_gy, 8, seq), f32),
        vmem((seq, slice_width), bf16),
        vmem((chunks, seq, block_width), bf16),
        vmem((n_gx, seq, quarter), bf16),
        vmem((2, 2, seq, quarter), bf16),
        vmem((2, seq, quarter), f32),
        vmem((2, seq, quarter), bf16),
        vmem((chunks, seq, quarter), bf16),
        vmem((3, seq, ff_cols), bf16),
        vmem((3, seq, head_cols), bf16),
        vmem((3, 2, 2, seq, slice_width), bf16),
        vmem((2, seq, slice_width), bf16),
        vmem((7, seq, slice_width), bf16),
        vmem((4, seq, slice_width), bf16),
        vmem((4, seq, slice_width), bf16),
        vmem((4, seq, slice_width), bf16),
        vmem((2, seq, slice_width), bf16),
        vmem((2, seq, slice_width), bf16),
        vmem((2, 2, seq, slice_width), bf16),
        dma((n_gx, 8)),
        dma((2, n_gx)),
        dma((2, n_gx)),
        dma((2,)),
        dma((n_gy,)),
        dma((n_gy,)),
        dma((GATHER_PIECES,)),
        dma((chunks, GATHER_PIECES)),
        dma((2, chunks, GATHER_PIECES)),
        dma((chunks, GATHER_PIECES)),
        dma((chunks, GATHER_PIECES)),
        dma((chunks, 2, 2)),
        dma((chunks, 2, 2)),
        dma((chunks, 2)),
        dma((chunks, 2)),
        dma((chunks, 3, 3)),
        dma((chunks, 3, 3)),
        dma((pieces,)),
        dma((pieces,)),
        dma((pieces,)),
        dma((pieces,)),
        dma((pieces,)),
        dma((4,)),
        dma((4,)),
        dma((8,)),
        dma((2, 8)),
        dma((4,)),
        pltpu.SemaphoreType.REGULAR,
        pltpu.SemaphoreType.REGULAR,
    ]
    in_vmem = pl.BlockSpec(memory_space=pltpu.VMEM)
    anywhere = pl.BlockSpec(memory_space=pl.ANY)
    return pl.pallas_call(
        functools.partial(block_kernel, n_gy),
        out_shape=jax.ShapeDtypeStruct(tokens.shape, bf16),
        in_specs=[in_vmem] * 4 + [anywhere] * 6,
        out_specs=in_vmem,
        scratch_shapes=scratch,
        compiler_params=pltpu.CompilerParams(
            collective_id=0, has_side_effects=True, vmem_limit_bytes=VMEM_LIMIT
        ),
    )(
        tokens,
        norm_gain.reshape(n_gy, 1, slice_width),
        query_gain.reshape(1, head),
        key_gain.reshape(1, head),
        jnp.transpose(qkv_weight, (1, 0, 2)),
        up_weight,
        out_weight,
        down_weight,
        attention_keep,
        feedforward_keep,
    )


def dispatch(*arrays):
    n_gx, n_gy = lax.axis_size("gx"), lax.axis_size("gy")
    images, seq, slice_width = arrays[0].shape
    head_cols, ff_cols = arrays[2].shape[2], arrays[3].shape[1]
    head = arrays[4].shape[0]
    fits = (
        n_gx == 4
        and n_gy == 2 * n_gx
        and images == 1
        and head == 128
        and head_cols % (n_gx * head) == 0
        and ff_cols % (n_gx * 128) == 0
        and slice_width % 128 == 0
        and seq % 128 == 0
    )
    return fused(*arrays) if fits else per_device(*arrays)


def solution(mesh):
    in_specs = (
        P("gx", None, "gy"),
        P(),
        P("gx", None, "gy"),
        P("gx", "gy"),
        P(),
        P(),
        P("gy", "gx"),
        P("gy", "gx"),
        P("gx", None, "gy"),
        P("gx", None, "gy"),
    )
    out_specs = P("gx", None, "gy")
    return jax.shard_map(
        dispatch, mesh=mesh, in_specs=in_specs, out_specs=out_specs, check_vma=False
    )
```

```python
import functools

import jax
import jax.numpy as jnp
from jax import lax
from jax.experimental import pallas as pl
from jax.experimental.pallas import tpu as pltpu
from jax.sharding import PartitionSpec as P

epsilon = 1e-06
keep_scale = 1.0 / 0.9
UP_CHUNKS = 2

f32 = jnp.float32
bf16 = jnp.bfloat16


def layer_norm(values, gain):
    center = values - jnp.mean(values, axis=-1, keepdims=True)
    variance = jnp.mean(center * center, axis=-1, keepdims=True)
    return center * lax.rsqrt(variance + epsilon) * gain


def head_norm(values, gain):
    row_count = values.shape[0]
    shaped = values.reshape(row_count, -1, gain.shape[0])
    return layer_norm(shaped, gain).reshape(row_count, -1)


def mul(left, right):
    return jnp.dot(left, right, preferred_element_type=f32)


def swap(values, bit, n_gx):
    return lax.ppermute(values, "gx", [(i, i ^ bit) for i in range(n_gx)])


def scatter_sum(odd_rows, even_rows, weight, n_gx):
    received = swap(mul(odd_rows, weight).astype(bf16), 1, n_gx)
    total = mul(even_rows, weight).astype(bf16).astype(f32) + received.astype(f32)
    bit, width = 2, weight.shape[1]
    own_rows = 2 * odd_rows.shape[0] // n_gx
    while bit < n_gx:
        pairs = total.reshape(-1, 2, own_rows, width)
        received = swap(pairs[:, 1].astype(bf16), bit, n_gx)
        total = pairs[:, 0] + received.astype(f32)
        bit *= 2
    return total.reshape(own_rows, width)


def gather_pair(own, n_gx):
    held, bit = own, n_gx // 2
    while bit > 1:
        held = jnp.concatenate([held, swap(held, bit, n_gx)], axis=0)
        bit //= 2
    return held, swap(held, 1, n_gx)


def gather_order(n_gx):
    order, bit = [0], n_gx // 2
    while bit >= 1:
        order = order + [p ^ bit for p in order]
        bit //= 2
    return order


def ring_place(index, count):
    return jnp.where(index % 2 == 0, index // 2, count - 1 - index // 2)


def ring_gather(own, ring, place):
    n = len(ring)
    ahead = [(ring[r], ring[(r + 1) % n]) for r in range(n)]
    back = [(b, a) for a, b in ahead]
    forward, backward = [own], [own]
    for step in range(n // 2 - 1):
        forward.append(lax.ppermute(forward[-1], "gy", ahead))
        backward.append(lax.ppermute(backward[-1], "gy", back))
    half = own.shape[0] // 2
    far = jnp.concatenate(
        [
            lax.ppermute(forward[-1][:half], "gy", ahead),
            lax.ppermute(backward[-1][half:], "gy", back),
        ],
        axis=0,
    )
    return jnp.stack(forward + [far] + backward[:0:-1])


def ring_scatter(partial, ring, place):
    n = len(ring)
    half = partial.shape[1] // 2
    ahead = [(ring[r], ring[(r + 1) % n]) for r in range(n)]
    back = [(b, a) for a, b in ahead]

    def block(index, start):
        index = lax.rem(index + 2 * n, n)
        return lax.dynamic_slice(
            partial, (index, start, 0), (1, half, partial.shape[2])
        )[0]

    up, down = block(place - 1, 0), block(place + 1, half)
    for step in range(n - 1):
        came_up = lax.ppermute(up, "gy", ahead)
        came_down = lax.ppermute(down, "gy", back)
        up = came_up.astype(f32) + block(place - 2 - step, 0).astype(f32)
        down = came_down.astype(f32) + block(place + 2 + step, half).astype(f32)
        up, down = up.astype(bf16), down.astype(bf16)
    return jnp.concatenate([up, down], axis=0)


def per_device(
    tokens,
    norm_gain,
    qkv_weight,
    up_weight,
    query_gain,
    key_gain,
    out_weight,
    down_weight,
    attention_keep,
    feedforward_keep,
):
    n_gx, n_gy = lax.axis_size("gx"), lax.axis_size("gy")
    sub = n_gy // n_gx
    me = lax.axis_index("gx")
    ring = list(range(0, n_gy, 2)) + list(range(1, n_gy, 2))[::-1]
    place = ring_place(lax.axis_index("gy"), n_gy)
    images, seq_len, slice_width = tokens.shape
    own_rows = images * seq_len
    block_width = qkv_weight.shape[0]
    head_cols = qkv_weight.shape[2]
    head_size = query_gain.shape[0]

    flat = tokens.reshape(own_rows, slice_width)
    turned = lax.ppermute(
        flat,
        ("gx", "gy"),
        [
            (i * n_gy + k * sub + s, k * n_gy + i * sub + s)
            for i in range(n_gx)
            for k in range(n_gx)
            for s in range(sub)
        ],
    )
    gathered = ring_gather(turned, ring, place)

    wide = flat.astype(f32)
    mean = jnp.mean(wide, axis=1)
    squares = jnp.sum((wide - mean[:, None]) ** 2, axis=1)
    count, bit = slice_width, 1
    while bit < n_gy:
        pairs = [(i, i ^ bit) for i in range(n_gy)]
        other = lax.ppermute(jnp.stack([mean, squares]), "gy", pairs)
        squares = squares + other[1] + (0.5 * count) * (mean - other[0]) ** 2
        mean = 0.5 * (mean + other[0])
        count, bit = 2 * count, 2 * bit
    stats = jnp.stack([mean, lax.rsqrt(squares / count + epsilon)])[None]
    bit = 1
    while bit < n_gx:
        stats = jnp.concatenate([stats, swap(stats, bit, n_gx)], axis=0)
        bit *= 2
    gain = lax.dynamic_slice_in_dim(norm_gain, me * block_width, block_width, 0)

    def normed_rows(position):
        image = me ^ position
        rows = jnp.concatenate(
            [
                lax.dynamic_index_in_dim(
                    gathered,
                    lax.rem(place - ring_place(image * sub + s, n_gy) + n_gy, n_gy),
                    0,
                    keepdims=False,
                )
                for s in range(sub)
            ],
            axis=1,
        ).astype(f32)
        row_mean, row_scale = stats[position, 0], stats[position, 1]
        return ((rows - row_mean[:, None]) * row_scale[:, None] * gain).astype(bf16)

    odd_rows = jnp.concatenate([normed_rows(p) for p in range(1, n_gx, 2)], axis=0)
    even_rows = jnp.concatenate([normed_rows(p) for p in range(0, n_gx, 2)], axis=0)

    qkv_flat = qkv_weight.reshape(block_width, 3 * head_cols)
    united = scatter_sum(odd_rows, even_rows, qkv_flat, n_gx)
    up_cols = up_weight.shape[1] // UP_CHUNKS
    hidden = []
    for c in range(UP_CHUNKS):
        total = scatter_sum(
            odd_rows, even_rows, up_weight[:, c * up_cols : (c + 1) * up_cols], n_gx
        )
        hidden.append(jax.nn.gelu(total, approximate=False).astype(bf16))

    queries = head_norm(united[:, :head_cols], query_gain).astype(bf16)
    keys = head_norm(united[:, head_cols : 2 * head_cols], key_gain).astype(bf16)
    values = united[:, 2 * head_cols :].astype(bf16)
    query_grid = queries.reshape(images, seq_len, -1, head_size)
    key_grid = keys.reshape(images, seq_len, -1, head_size)
    value_grid = values.reshape(images, seq_len, -1, head_size)
    scores = jnp.einsum(
        "bshd,bthd->bhst", query_grid, key_grid, preferred_element_type=f32
    ) * head_size ** (-0.5)
    raised = jnp.exp(scores)
    weights = (raised / jnp.sum(raised, axis=-1, keepdims=True)).astype(bf16)
    attended = jnp.einsum("bhst,bthd->bshd", weights, value_grid, preferred_element_type=f32)
    attended = attended.astype(bf16).reshape(own_rows, head_cols)

    order = gather_order(n_gx)
    def home(devices):
        return [
            (
                k * n_gy + devices[s * n_gx + q],
                (k ^ order[q]) * n_gy + k * sub + s,
            )
            for k in range(n_gx)
            for s in range(sub)
            for q in range(n_gx)
        ]

    def columns(weight, s):
        return weight[:, s * slice_width : (s + 1) * slice_width]

    attended_halves = gather_pair(attended, n_gx)
    attention_out = lax.psum_scatter(
        jnp.concatenate(
            [
                mul(rows, columns(out_weight, s)).astype(bf16)
                for s in range(sub)
                for rows in attended_halves
            ],
            axis=0,
        ),
        "gy",
        scatter_dimension=0,
        tiled=True,
    )
    attention_out = lax.ppermute(attention_out, ("gx", "gy"), home(range(n_gy))).astype(f32)
    hidden_halves = [gather_pair(part, n_gx) for part in hidden]
    pieces = []
    for s in range(sub):
        for half in range(2):
            total = 0.0
            for c in range(UP_CHUNKS):
                weight = down_weight[c * up_cols : (c + 1) * up_cols]
                total = total + mul(hidden_halves[c][half], columns(weight, s))
            pieces.append(total.astype(bf16))
    partial = jnp.concatenate(pieces, axis=0).reshape(n_gy, own_rows, slice_width)
    feedforward_out = ring_scatter(partial, ring, place)
    feedforward_out = lax.ppermute(feedforward_out, ("gx", "gy"), home(ring)).astype(f32)

    shape = tokens.shape
    branches = attention_keep.astype(f32) * attention_out.reshape(
        shape
    ) + feedforward_keep.astype(f32) * feedforward_out.reshape(shape)
    return (tokens.astype(f32) + branches * keep_scale).astype(bf16)


MESH = pl.DeviceIdType.MESH
VMEM_LIMIT = 67043328
GATHER_PIECES = 4
ROW_STEP = 64
FIRST_SECTIONS = 1


def flip(index, mask):
    for bit in (1, 2):
        if mask & bit:
            index = index + bit - 2 * bit * ((index // bit) % 2)
    return index


SCHEDULE = (
    "mark0", "relay0", "relay1", "relay2/root", "relay3/root", "gather0", "exchange0",
    "relay2/mid", "exchange1", "masks2/root", "masks0/root", "relay3/mid", "activate0",
    "masks2/near", "masks1/root", "gather3", "exchange2", "activate1", "masks0/near",
    "forward0", "finish0", "masks2/far", "masks1/near", "reduce0/0", "activate2", "exchange3",
    "masks0/far", "reduce1/0", "reduce0/1", "forward1", "finish1", "masks1/far", "reduce1/1",
    "reduce0/2", "forward2", "finish2", "reduce2/0", "reduce3/0", "reduce1/2", "activate3",
    "reduce2/1", "reduce0/3", "reduce1/3", "reduce3/1", "reduce2/2", "forward3", "masks2/end",
    "reduce4/0", "reduce5/0", "masks0/end", "masks1/end", "finish3", "reduce4/1", "close3", "reduce3/2",
    "reduce2/3", "reduce3/3", "reduce4/2", "reduce4/3", "reduce5/late", "reduce6", "reduce7",
)


def schedule():
    for word in SCHEDULE:
        name, _, role = word.partition("/")
        yield name[:-1], int(name[-1]), role


def remote(src, dst, send_sem, recv_sem, device):
    return pltpu.make_async_remote_copy(
        src_ref=src,
        dst_ref=dst,
        send_sem=send_sem,
        recv_sem=recv_sem,
        device_id=device,
        device_id_type=MESH,
    )


scope = jax.named_scope


def over_rows(count, body):
    def step(i, carry):
        body(pl.ds(pl.multiple_of(i * ROW_STEP, ROW_STEP), ROW_STEP))
        return carry

    lax.fori_loop(0, count // ROW_STEP, step, 0)


def aligned(start, size):
    return pl.ds(pl.multiple_of(start, size), size)


def block_kernel(
    n_gy,
    tokens,
    gain,
    query_gain,
    key_gain,
    qkv_hbm,
    up_hbm,
    out_hbm,
    down_hbm,
    attention_keep,
    feedforward_keep,
    result,
    *scratch,
):
    (
        w_in,
        w_down,
        w_out,
        keeps,
        stat_own,
        stat_all,
        normed,
        rows_in,
        part,
        part_in,
        kept,
        cross,
        cross_in,
        hid,
        att,
        branch,
        merged,
        branch_in,
        line_out,
        line_low,
        line_high,
        final,
        mask_own,
        mask_in,
        in_sem,
        down_sem,
        out_sem,
        keep_sem,
        stat_send,
        stat_recv,
        first_send,
        gather_recv,
        gather_send,
        side_send,
        side_recv,
        part_send,
        part_recv,
        cross_send,
        cross_recv,
        share_send,
        share_recv,
        branch_send,
        branch_recv,
        line_send,
        low_recv,
        high_recv,
        final_recv,
        mask_first,
        mask_recv,
        mask_send,
        mask_side,
        line_credit,
        turn,
    ) = scratch
    n_gx = 4
    sub = n_gy // n_gx
    g, j = lax.axis_index("gx"), lax.axis_index("gy")
    z, x = j // sub, j % sub
    core, across, side = (flip(g, 1), j), (flip(g, 2), j), (g, j + 1 - 2 * x)
    seq, slice_width = normed.shape
    features = n_gy * slice_width
    head = query_gain.shape[1]
    quarter_head, quarter_ff = att.shape[2] // n_gx, hid.shape[2] // n_gx
    quarter = part.shape[2]
    chunks = n_gx
    step_rows = seq // GATHER_PIECES
    own_cols, side_cols = pl.ds(0, slice_width), pl.ds(slice_width, slice_width)

    relative = (3, 2, 1, 0)
    in_copies, down_copies, out_copies = [], [], []
    for q, r in enumerate(relative):
        k = flip(g, r)
        copies = []
        for h in range(2):
            from_rows = aligned(slice_width * (x if h == 0 else 1 - x), slice_width)
            to_rows = pl.ds(h * slice_width, slice_width)
            for t in range(3):
                copies.append(
                    (
                        qkv_hbm.at[t, from_rows, aligned(k * quarter_head, quarter_head)],
                        w_in.at[q, to_rows, pl.ds(t * quarter_head, quarter_head)],
                    )
                )
            copies.append(
                (
                    up_hbm.at[from_rows, aligned(k * quarter_ff, quarter_ff)],
                    w_in.at[q, to_rows, pl.ds(3 * quarter_head, quarter_ff)],
                )
            )
        in_copies.append(
            [
                pltpu.make_async_copy(a, b, in_sem.at[q, n])
                for n, (a, b) in enumerate(copies)
            ]
        )
    for s in range(2):
        from_cols = aligned(slice_width * (1 - x if s == 0 else x), slice_width)
        for r in range(n_gx):
            k = flip(g, r)
            down_copies.append(
                pltpu.make_async_copy(
                    down_hbm.at[aligned(k * quarter_ff, quarter_ff), from_cols],
                    w_down.at[s, pl.ds(r * quarter_ff, quarter_ff)],
                    down_sem.at[s, r],
                )
            )
            out_copies.append(
                pltpu.make_async_copy(
                    out_hbm.at[aligned(k * quarter_head, quarter_head), from_cols],
                    w_out.at[s, pl.ds(r * quarter_head, quarter_head)],
                    out_sem.at[s, r],
                )
            )
    keep_copies = [
        pltpu.make_async_copy(attention_keep, keeps.at[0], keep_sem.at[0]),
        pltpu.make_async_copy(feedforward_keep, keeps.at[1], keep_sem.at[1]),
    ]
    mark_scope = scope('begin')
    mark_scope.__enter__()
    for copies in in_copies:
        for copy in copies:
            copy.start()
    for copy in down_copies + out_copies + keep_copies:
        copy.start()

    barrier = pltpu.get_barrier_semaphore()
    for r in range(1, n_gx):
        pl.semaphore_signal(
            barrier, inc=1, device_id=(flip(g, r), j), device_id_type=MESH
        )
    for d in range(1, n_gy):
        pl.semaphore_signal(
            barrier, inc=1, device_id=(g, (j + d) % n_gy), device_id_type=MESH
        )

    mark_scope.__exit__(None, None, None)
    mark_scope = scope('moments')
    mark_scope.__enter__()
    wide = tokens[0].astype(f32)
    mean = jnp.mean(wide, axis=1, keepdims=True)
    squares = jnp.sum((wide - mean) ** 2, axis=1, keepdims=True)
    mean_row = jnp.transpose(jnp.broadcast_to(mean, (seq, 128)))[:8]
    squares_row = jnp.transpose(jnp.broadcast_to(squares, (seq, 128)))[:8]
    top = lax.broadcasted_iota(jnp.int32, (8, seq), 0) == 0
    stats = jnp.where(top, mean_row, squares_row)
    stat_own[...] = stats
    stat_all[0] = stats
    mark_scope.__exit__(None, None, None)
    mark_scope = scope('barrier')
    mark_scope.__enter__()
    pl.semaphore_wait(barrier, n_gx + n_gy - 2)
    mark_scope.__exit__(None, None, None)
    mark_scope = scope('swap')
    mark_scope.__enter__()
    stat_copies = [
        remote(
            stat_own,
            stat_all.at[d],
            stat_send.at[d],
            stat_recv.at[d],
            (g, (j + d) % n_gy),
        )
        for d in range(1, n_gy)
    ]
    for copy in stat_copies:
        copy.start()
    for copy in stat_copies:
        copy.wait_recv()
    mark_scope.__exit__(None, None, None)
    mark_scope = scope('norm')
    mark_scope.__enter__()
    means = [stat_all[d, 0:1] for d in range(n_gy)]
    total_mean = sum(means) * (1.0 / n_gy)
    spread = sum((m - total_mean) ** 2 for m in means) * float(slice_width)
    spread = spread + sum(stat_all[d, 1:2] for d in range(n_gy))
    scale = lax.rsqrt(spread * (1.0 / features) + epsilon)
    mean_col = jnp.transpose(jnp.broadcast_to(total_mean, (128, seq)))
    scale_col = jnp.transpose(jnp.broadcast_to(scale, (128, seq)))
    for c0 in range(0, slice_width, 128):
        cols = slice(c0, c0 + 128)
        centre = tokens[0, :, cols].astype(f32) - mean_col
        normed[:, cols] = (centre * scale_col * gain[j, :, cols]).astype(bf16)

    at_root = g == z
    first_copies = [
        remote(
            normed.at[pl.ds(p * step_rows, step_rows)],
            rows_in.at[g, pl.ds(p * step_rows, step_rows), own_cols],
            first_send.at[p],
            gather_recv.at[g, p],
            (z, j),
        )
        for p in range(GATHER_PIECES)
    ]

    @pl.when(at_root)
    def _():
        rows_in[g, :, own_cols] = normed[...]

    mark_scope.__exit__(None, None, None)
    @pl.when(g % 2 == 1)
    def _():
        pl.semaphore_wait(turn, 1)

    @pl.when(jnp.logical_not(at_root))
    def _():
        for copy in first_copies:
            copy.start()

    @pl.when(g % 2 == 0)
    def _():
        @pl.when(jnp.logical_not(at_root))
        def _():
            for copy in first_copies:
                copy.wait_send()

        pl.semaphore_signal(turn, inc=1, device_id=core, device_id_type=MESH)

    join, fuse = chunks - 1, chunks - 2
    half_rows = seq // 2

    def mask_ref(i):
        return mask_in.at[i // 4, i // 2 % 2, pl.ds(i % 2 * half_rows, half_rows)]

    mask_slot = 2 * (join - g)

    def mask_first_copy(i):
        part_of = (i // 2, pl.ds(i % 2 * half_rows, half_rows))
        return remote(
            mask_own.at[part_of],
            mask_in.at[(mask_slot, *part_of)],
            mask_first.at[i],
            mask_recv.at[4 * mask_slot + i],
            (z, j),
        )

    def mark(_):
        @pl.when(g >= fuse)
        def _():
            for b in range(2):
                keep_copies[b].wait()

                def to_mask(rows):
                    mask_own[b, rows] = keeps[b, 0, rows].astype(f32).astype(bf16)

                over_rows(seq, to_mask)

            @pl.when(at_root)
            def _():
                mask_in[mask_slot] = mask_own[...]

            @pl.when(jnp.logical_not(at_root))
            def _():
                for i in range(4):
                    mask_first_copy(i).start()

    goes_down = jnp.logical_and(z <= g, z > 0)
    goes_up = jnp.logical_and(z >= g, z < n_gx - 1)
    duty = jnp.logical_or(goes_down, goes_up)

    def mask_copies(i):
        own = mask_ref(i)
        down = remote(own, own, mask_send.at[0, i], mask_recv.at[i], (g, j - sub))
        up = remote(own, own, mask_send.at[1, i], mask_recv.at[i], (g, j + sub))
        return down, up

    def mask_beside(i):
        return remote(
            mask_ref(i), mask_ref(4 + i), mask_side.at[i], mask_recv.at[4 + i], side
        )

    def masks(s):
        for i in range(4 * s, 4 * s + 4):
            down, up = mask_copies(i)
            if s == 1:
                up.wait_recv()
            else:
                image = join if s == 0 else fuse

                @pl.when(jnp.logical_not(jnp.logical_and(at_root, g == image)))
                def _():
                    up.wait_recv()

            if s == 0:

                @pl.when(at_root)
                def _():
                    mask_beside(i).start()

            @pl.when(goes_up)
            def _():
                up.start()

            @pl.when(goes_down)
            def _():
                down.start()

    def gather_ref(c, p, cols):
        return rows_in.at[c, pl.ds(p * step_rows, step_rows), cols]

    def gather_copies(c, p):
        own = gather_ref(c, p, own_cols)
        down = remote(
            own, own, gather_send.at[0, c, p], gather_recv.at[c, p], (g, j - sub)
        )
        up = remote(
            own, own, gather_send.at[1, c, p], gather_recv.at[c, p], (g, j + sub)
        )
        beside = remote(
            own,
            gather_ref(c, p, side_cols),
            side_send.at[c, p],
            side_recv.at[c, p],
            side,
        )
        return down, up, beside

    def gather(c, pieces=range(GATHER_PIECES)):
        for p in pieces:
            down, up, beside = gather_copies(c, p)

            @pl.when(jnp.logical_not(jnp.logical_and(at_root, g == c)))
            def _():
                up.wait_recv()

            @pl.when(goes_up)
            def _():
                up.start()

            @pl.when(goes_down)
            def _():
                down.start()

            beside.start()

    def gathered(c, pieces):
        for p in pieces:
            gather_copies(c, p)[2].wait_recv()

    def sections(c):
        count = FIRST_SECTIONS if c == 0 else 1
        return [
            (sec, slice(sec * seq // count, (sec + 1) * seq // count))
            for sec in range(count)
        ]

    def part_copy(c, half, section):
        sec, rows = section
        return remote(
            part.at[2 * half, rows],
            part_in.at[c % 2, half, rows],
            part_send.at[c, half, sec],
            part_recv.at[c, half, sec],
            core,
        )

    def cross_copy(c, section):
        sec, rows = section
        return remote(
            cross.at[c % 2, rows],
            cross_in.at[c, rows],
            cross_send.at[c, sec],
            cross_recv.at[c, sec],
            across,
        )

    def project(c, half, section):
        rows = section[1]
        if c == 0 and section[0] == 0:
            for copy in in_copies[2 * half] + in_copies[2 * half + 1]:
                copy.wait()
        if c > 0:
            for earlier in sections(c - 1):
                part_copy(c - 1, half, earlier).wait_send()

        def one(i, carry):
            q = 2 * half + i
            for n0 in range(0, quarter, 256):
                n1 = min(n0 + 256, quarter)
                part[q, rows, n0:n1] = mul(
                    rows_in[c, rows], w_in[q, :, n0:n1]
                ).astype(bf16)

            @pl.when(i == 0)
            def _():
                part_copy(c, half, section).start()

            return carry

        lax.fori_loop(0, 2, one, 0)

    def exchange(c):
        if c >= slots:
            for unit in range(3):
                share_copies(c - slots, unit)[2].wait_send()
        if c >= 2:
            for earlier in sections(c - 2):
                cross_copy(c - 2, earlier).wait_send()
        for section in sections(c):
            rows = section[1]
            pieces = range(rows.start // step_rows, rows.stop // step_rows)
            gathered(c, pieces)
            project(c, 0, section)
            part_copy(c, 0, section).wait_recv()

            def to_cross(step):
                here = pl.ds(rows.start + step.start, ROW_STEP)
                total = part[1, here].astype(f32) + part_in[c % 2, 0, here].astype(f32)
                cross[c % 2, here] = total.astype(bf16)

            over_rows(rows.stop - rows.start, to_cross)
            cross_copy(c, section).start()
            half_pieces = GATHER_PIECES // 2
            if c < 2:
                early = range(half_pieces)
                pl.when(jnp.logical_not(duty))(functools.partial(gather, c + 1, early))
            project(c, 1, section)
            if c < 2:
                late = range(half_pieces, GATHER_PIECES)
                pl.when(jnp.logical_not(duty))(functools.partial(gather, c + 1, late))
            part_copy(c, 1, section).wait_recv()

            def to_kept(step):
                here = pl.ds(rows.start + step.start, ROW_STEP)
                kept[c % 2, here] = part[3, here].astype(f32) + part_in[
                    c % 2, 1, here
                ].astype(f32)

            over_rows(rows.stop - rows.start, to_kept)

    slots = hid.shape[0]
    half_rows = seq // 2

    def half_of(h):
        return slice(h * half_rows, (h + 1) * half_rows)

    def share_copies(c, unit):
        held, width = (hid, quarter_ff) if unit < 2 else (att, quarter_head)
        rows = half_of(unit) if unit < 2 else slice(0, seq)

        def slot(r):
            return held.at[c % slots, rows, pl.ds(r * width, width)]

        return [
            remote(
                slot(a),
                slot(b),
                share_send.at[c, unit, n],
                share_recv.at[c, unit, n],
                device,
            )
            for n, (a, b, device) in enumerate(
                ((0, 2, across), (0, 1, core), (2, 3, core))
            )
        ]

    def share(c, unit):
        to_across, to_core, _ = share_copies(c, unit)
        to_across.start()
        to_core.start()

    def activate(c):
        if c >= slots:
            for unit in range(3):
                for copy in share_copies(c - slots, unit)[:2]:
                    copy.wait_send()
        for section in sections(c):
            cross_copy(c, section).wait_recv()
        order = (2, 0, 1) if c >= join else (0, 1, 2)
        for unit in order:
            if unit == 2:
                attend(c)
            else:
                activate_rows(c, unit * half_rows)
            share(c, unit)

    def activate_rows(c, offset):
        first = 3 * quarter_head

        def to_hidden(step):
            rows = pl.ds(offset + step.start, ROW_STEP)
            total = kept[c % 2, rows, first:] + cross_in[c, rows, first:].astype(f32)
            hid[c % slots, rows, 0:quarter_ff] = (
                0.5 * total * (1.0 + lax.erf(total * (0.5**0.5)))
            ).astype(bf16)

        over_rows(half_rows, to_hidden)

    def attend(c):
        for h in range(quarter_head // head):

            def of(t):
                cols = slice(t * quarter_head + h * head, t * quarter_head + (h + 1) * head)
                return kept[c % 2, :, cols] + cross_in[c, :, cols].astype(f32)

            query = layer_norm(of(0), query_gain[...]).astype(bf16)
            key = layer_norm(of(1), key_gain[...]).astype(bf16)
            value = of(2).astype(bf16)
            scores = lax.dot_general(
                query, key, (((1,), (1,)), ((), ())), preferred_element_type=f32
            ) * head ** (-0.5)
            raised = jnp.exp(scores)
            weights = (raised / jnp.sum(raised, axis=-1, keepdims=True)).astype(bf16)
            att[c % slots, :, h * head : (h + 1) * head] = mul(weights, value).astype(
                bf16
            )

    def onward(c, unit):
        from_across, _, to_core = share_copies(c, unit)
        from_across.wait_recv()
        to_core.start()

    def forward(c):
        for unit in (2, 0) if c >= join else (0, 1, 2):
            onward(c, unit)

    quarter_rows = seq // 4

    def piece_rows(p):
        if p // 4 < join:
            return slice(p % 2 * half_rows, (p % 2 + 1) * half_rows)
        return slice(p % 4 * quarter_rows, (p % 4 + 1) * quarter_rows)

    def piece_slot(p):
        return p // 2 if p // 4 < join else 2 * join

    def line_slot(p):
        return p // 2 % 4

    def sum_rows(p):
        if p // 4 < fuse:
            return piece_rows(p)
        return slice(p % 4 * quarter_rows, (p % 4 + 1) * quarter_rows)

    def line_rows(p):
        rows = sum_rows(p)
        start = p % 2 * half_rows
        return slice(start, start + rows.stop - rows.start)

    def branch_ref(p, s):
        c, b, rows = p // 4, p // 2 % 2, piece_rows(p)
        return branch.at[c, b, s, rows] if c < join else merged.at[s, rows]

    def branch_copy(p):
        return remote(
            branch_ref(p, 0),
            branch_in.at[piece_slot(p), piece_rows(p)],
            branch_send.at[p],
            branch_recv.at[p],
            side,
        )

    def shares_arrive(c, unit):
        for copy in share_copies(c, unit)[1:]:
            copy.wait_recv()
        if c == 0 and unit > 0:
            for copy in (down_copies, out_copies)[unit - 1]:
                copy.wait()

    def finish(c):
        if c >= join:
            finish_joined(c, 0)
            onward(c, 1)
            return
        for b, held, weight in ((0, att, w_out), (1, hid, w_down)):
            for unit in (2,) if b == 0 else (0, 1):
                shares_arrive(c, unit)

            def one(s, carry):
                for n0 in range(0, slice_width, 256):
                    n1 = min(n0 + 256, slice_width)
                    branch[c, b, s, :, n0:n1] = mul(
                        held[c % slots], weight[s, :, n0:n1]
                    ).astype(bf16)

                @pl.when(s == 0)
                def _():
                    for h in range(2):
                        branch_copy(4 * c + 2 * b + h).start()

                return carry

            lax.fori_loop(0, 2, one, 0)

    def finish_joined(c, h):
        if h == 0:
            shares_arrive(c, 2)
        shares_arrive(c, h)
        rows = half_of(h)

        def one(s, carry):
            for n0 in range(0, slice_width, 256):
                cols = slice(n0, min(n0 + 256, slice_width))
                keep_att = mask_in[1 - s, 0, rows, cols].astype(f32)
                keep_ff = mask_in[1 - s, 1, rows, cols].astype(f32)
                total = keep_att * mul(att[c % slots, rows], w_out[s, :, cols])
                total = total + keep_ff * mul(hid[c % slots, rows], w_down[s, :, cols])
                merged[s, rows, cols] = total.astype(bf16)

            @pl.when(s == 0)
            def _():
                for i in range(2):
                    branch_copy(4 * c + 2 * h + i).start()

            return carry

        lax.fori_loop(0, 2, one, 0)

    def close(c):
        finish_joined(c, 1)

    from_low = jnp.logical_and(z <= g, z > 0)
    from_high = jnp.logical_and(z >= g, z < n_gx - 1)
    below, above = z < g, z > g

    def line_copies(p):
        c = p // 4
        k, rows, held = line_slot(p), sum_rows(p), line_rows(p)
        own = line_out.at[k, held]
        up = remote(
            own, line_low.at[k, held], line_send.at[p], low_recv.at[p], (g, j + sub)
        )
        down = remote(
            own, line_high.at[k, held], line_send.at[p], high_recv.at[p], (g, j - sub)
        )
        landing = final.at[p // 2 % 2 if c < fuse else 0, rows]
        home = remote(own, landing, line_send.at[p], final_recv.at[p % 4], (c, j))
        return up, down, home

    def leaves(p):
        return jnp.logical_not(jnp.logical_and(at_root, g == p // 4))

    def reduce(n):
        for p in (2 * n, 2 * n + 1):
            reduce_piece(p)

    def reduce_piece(p):
        c = p // 4
        k, rows = line_slot(p), sum_rows(p)
        count, offset = rows.stop - rows.start, rows.start
        shift = line_rows(p).start
        up, down, home = line_copies(p)
        if c < fuse or c >= join:
            branch_copy(p).wait_recv()
        elif p % 2 == 0:
            for b in range(2):
                branch_copy(4 * c + 2 * b + p // 2 % 2).wait_recv()

        @pl.when(from_low)
        def _():
            up.wait_recv()

        @pl.when(from_high)
        def _():
            down.wait_recv()

        if p >= 8:

            @pl.when(leaves(p - 8))
            def _():
                line_copies(p - 8)[0].wait_send()

            @pl.when(jnp.logical_not(at_root))
            def _():
                pl.semaphore_wait(line_credit, 1)

        def total_rows(step):
            here = pl.ds(offset + step.start, ROW_STEP)
            if c < fuse or c >= join:
                total = branch_ref(p, 1)[step].astype(f32) + branch_in[
                    piece_slot(p), here
                ].astype(f32)
            else:
                total = 0.0
                for b in range(2):
                    both = branch[c, b, 1, here].astype(f32) + branch_in[
                        2 * c + b, here
                    ].astype(f32)
                    total = total + mask_in[2, b, here].astype(f32) * both
            low = line_low[k, pl.ds(shift + step.start, ROW_STEP)].astype(f32)
            high = line_high[k, pl.ds(shift + step.start, ROW_STEP)].astype(f32)
            total = total + jnp.where(from_low, low, 0.0)
            total = total + jnp.where(from_high, high, 0.0)
            line_out[k, pl.ds(shift + step.start, ROW_STEP)] = total.astype(bf16)

        over_rows(count, total_rows)
        if p < 8:
            for here, source in ((from_low, j - sub), (from_high, j + sub)):

                @pl.when(here)
                def _():
                    pl.semaphore_signal(
                        line_credit, inc=1, device_id=(g, source), device_id_type=MESH
                    )

        @pl.when(below)
        def _():
            up.start()

        @pl.when(above)
        def _():
            down.start()

        @pl.when(at_root)
        def _():
            @pl.when(g == c)
            def _():
                final[p // 2 % 2 if c < fuse else 0, rows] = line_out[k, line_rows(p)]

            @pl.when(g != c)
            def _():
                home.start()

    steps = dict(
        relay=gather,
        gather=gather,
        masks=masks,
        mark=mark,
        exchange=exchange,
        activate=activate,
        forward=forward,
        finish=finish,
        close=close,
        reduce=reduce,
    )
    hops = jnp.where(at_root, 3, jnp.where(below, z, n_gx - 1 - z))
    roles = {
        "relay": duty,
        "gather": jnp.logical_not(duty),
        "root": at_root,
        "mid": jnp.logical_and(duty, jnp.logical_not(at_root)),
        "near": jnp.logical_and(duty, jnp.abs(z - g) == 1),
        "far": jnp.logical_and(duty, jnp.abs(z - g) > 1),
        "end": jnp.logical_not(duty),
        "late": hops > 0,
    }
    for d in range(n_gx):
        roles[str(d)] = hops == d
    for act, c, role in schedule():
        with scope(f"{act}{c}"):
            step = functools.partial(steps[act], c)
            if role or act in ("relay", "gather"):
                pl.when(roles[role or act])(step)
            else:
                step()

    def arrive(p):
        @pl.when(jnp.logical_not(at_root))
        def _():
            line_copies(p)[2].wait_recv()

    @pl.when(g < fuse)
    def _():
        for b in range(2):
            keep_copies[b].wait()
        for p in range(4):
            arrive(p)

        def last(rows):
            total = keeps[0, 0, rows].astype(f32) * final[0, rows].astype(f32)
            total = total + keeps[1, 0, rows].astype(f32) * final[1, rows].astype(f32)
            result[0, rows] = (
                tokens[0, rows].astype(f32) + total * keep_scale
            ).astype(bf16)

        over_rows(seq, last)

    @pl.when(g >= fuse)
    def _():
        for p in range(4):
            arrive(4 * join + p)

        def last(rows):
            total = final[0, rows].astype(f32)
            result[0, rows] = (
                tokens[0, rows].astype(f32) + total * keep_scale
            ).astype(bf16)

        over_rows(seq, last)

        @pl.when(jnp.logical_not(at_root))
        def _():
            for i in range(4):
                mask_first_copy(i).wait_send()

    @pl.when(at_root)
    def _():
        for i in range(4):
            mask_beside(i).wait_send()

    for i in range(12):
        down, up = mask_copies(i)

        @pl.when(goes_up)
        def _():
            up.wait_send()

        @pl.when(goes_down)
        def _():
            down.wait_send()

    for copy in stat_copies:
        copy.wait_send()

    @pl.when(jnp.logical_and(jnp.logical_not(at_root), g % 2 == 1))
    def _():
        for copy in first_copies:
            copy.wait_send()

    for c in range(chunks):
        for p in range(GATHER_PIECES):
            down, up, beside = gather_copies(c, p)
            beside.wait_send()

            @pl.when(goes_up)
            def _():
                up.wait_send()

            @pl.when(goes_down)
            def _():
                down.wait_send()

        for unit in range(3) if c >= chunks - slots else []:
            for copy in share_copies(c, unit):
                copy.wait_send()
    for half in range(2):
        for section in sections(chunks - 1):
            part_copy(chunks - 1, half, section).wait_send()
    for c in range(chunks - 2, chunks):
        for section in sections(c):
            cross_copy(c, section).wait_send()
    for p in range(8):
        branch_copy(p).wait_send()
    for p in range(8, 16):
        branch_copy(p).wait_send()

        @pl.when(leaves(p))
        def _():
            line_copies(p)[0].wait_send()


def fused(
    tokens,
    norm_gain,
    qkv_weight,
    up_weight,
    query_gain,
    key_gain,
    out_weight,
    down_weight,
    attention_keep,
    feedforward_keep,
):
    n_gx, n_gy = lax.axis_size("gx"), lax.axis_size("gy")
    _, seq, slice_width = tokens.shape
    block_width, _, head_cols = qkv_weight.shape
    ff_cols = up_weight.shape[1]
    head = query_gain.shape[0]
    quarter_head, quarter_ff = head_cols // n_gx, ff_cols // n_gx
    quarter = 3 * quarter_head + quarter_ff
    chunks, pieces = n_gx, 4 * n_gx
    dma, vmem = pltpu.SemaphoreType.DMA, pltpu.VMEM
    scratch = [
        vmem((n_gx, block_width, quarter), bf16),
        vmem((2, ff_cols, slice_width), bf16),
        vmem((2, head_cols, slice_width), bf16),
        vmem((2, 1, seq, slice_width), jnp.int32),
        vmem((8, seq), f32),
        vmem((n_gy, 8, seq), f32),
        vmem((seq, slice_width), bf16),
        vmem((chunks, seq, block_width), bf16),
        vmem((n_gx, seq, quarter), bf16),
        vmem((2, 2, seq, quarter), bf16),
        vmem((2, seq, quarter), f32),
        vmem((2, seq, quarter), bf16),
        vmem((chunks, seq, quarter), bf16),
        vmem((3, seq, ff_cols), bf16),
        vmem((3, seq, head_cols), bf16),
        vmem((3, 2, 2, seq, slice_width), bf16),
        vmem((2, seq, slice_width), bf16),
        vmem((7, seq, slice_width), bf16),
        vmem((4, seq, slice_width), bf16),
        vmem((4, seq, slice_width), bf16),
        vmem((4, seq, slice_width), bf16),
        vmem((2, seq, slice_width), bf16),
        vmem((2, seq, slice_width), bf16),
        vmem((3, 2, seq, slice_width), bf16),
        dma((n_gx, 8)),
        dma((2, n_gx)),
        dma((2, n_gx)),
        dma((2,)),
        dma((n_gy,)),
        dma((n_gy,)),
        dma((GATHER_PIECES,)),
        dma((chunks, GATHER_PIECES)),
        dma((2, chunks, GATHER_PIECES)),
        dma((chunks, GATHER_PIECES)),
        dma((chunks, GATHER_PIECES)),
        dma((chunks, 2, 2)),
        dma((chunks, 2, 2)),
        dma((chunks, 2)),
        dma((chunks, 2)),
        dma((chunks, 3, 3)),
        dma((chunks, 3, 3)),
        dma((pieces,)),
        dma((pieces,)),
        dma((pieces,)),
        dma((pieces,)),
        dma((pieces,)),
        dma((4,)),
        dma((4,)),
        dma((12,)),
        dma((2, 12)),
        dma((4,)),
        pltpu.SemaphoreType.REGULAR,
        pltpu.SemaphoreType.REGULAR,
    ]
    in_vmem = pl.BlockSpec(memory_space=pltpu.VMEM)
    anywhere = pl.BlockSpec(memory_space=pl.ANY)
    return pl.pallas_call(
        functools.partial(block_kernel, n_gy),
        out_shape=jax.ShapeDtypeStruct(tokens.shape, bf16),
        in_specs=[in_vmem] * 4 + [anywhere] * 6,
        out_specs=in_vmem,
        scratch_shapes=scratch,
        compiler_params=pltpu.CompilerParams(
            collective_id=0, has_side_effects=True, vmem_limit_bytes=VMEM_LIMIT
        ),
    )(
        tokens,
        norm_gain.reshape(n_gy, 1, slice_width),
        query_gain.reshape(1, head),
        key_gain.reshape(1, head),
        jnp.transpose(qkv_weight, (1, 0, 2)),
        up_weight,
        out_weight,
        down_weight,
        attention_keep,
        feedforward_keep,
    )


def dispatch(*arrays):
    n_gx, n_gy = lax.axis_size("gx"), lax.axis_size("gy")
    images, seq, slice_width = arrays[0].shape
    head_cols, ff_cols = arrays[2].shape[2], arrays[3].shape[1]
    head = arrays[4].shape[0]
    fits = (
        n_gx == 4
        and n_gy == 2 * n_gx
        and images == 1
        and head == 128
        and head_cols % (n_gx * head) == 0
        and ff_cols % (n_gx * 128) == 0
        and slice_width % 128 == 0
        and seq % 128 == 0
    )
    return fused(*arrays) if fits else per_device(*arrays)


def solution(mesh):
    in_specs = (
        P("gx", None, "gy"),
        P(),
        P("gx", None, "gy"),
        P("gx", "gy"),
        P(),
        P(),
        P("gy", "gx"),
        P("gy", "gx"),
        P("gx", None, "gy"),
        P("gx", None, "gy"),
    )
    out_specs = P("gx", None, "gy")
    return jax.shard_map(
        dispatch, mesh=mesh, in_specs=in_specs, out_specs=out_specs, check_vma=False
    )
```
